256 devices in a mesh: batch: 8 (over x, core), seq: 32 (over y, z).
Axes of the slice: x: 4, y: 4, z: 8, core: 2. Of those that a mesh axis runs over, the one named last changes fastest.
Arguments:
- cotangent: bfloat16 [8, 4096, 4096], P('batch', 'seq'), may hold values from -23 to 23
- fixed_point: bfloat16 [8, 4096, 4096], P('batch', 'seq'), may hold values from -6 to 6
- input_map: bfloat16 [8, 4096, 128], P('batch', 'seq'), may hold values from -0.00390625 to 0.00390625
- output_map: bfloat16 [8, 4096, 128], P('batch', 'seq'), may hold values from -6 to 6
- step_size: float32 [8, 64, 4096], P('batch', None, 'seq'), may hold values from 0.3 to 3.4
- forget: float32 [8, 4096], P('batch', 'seq'), may hold values from 0 to 1, as said below
- decay_rate: float32 [64], replicated, may hold values from 4.8828125e-06 to 0.04
- skip_gain: float32 [64], replicated, may hold values from 0.3 to 0.65
Outputs:
- adjoint_sum: bfloat16 [8, 4096, 4096], P('batch', 'seq')
- rate_grad: float32 [64], replicated
- skip_grad: float32 [64], replicated
The draws below stay inside these ranges and needn't reach their ends.
Inputs may be any that keep to these rules, and one draw needn't show every extreme that they name: `forget`: nonzero at few positions.
All inputs are finite; a program needn't handle non-finite values.
Results may differ from the reference program's by a relative error of at most 0.034.
Values may be sent and summed in bfloat16 or wider, within the bound.
No kernel may reach another device: no remote copies, remote signals or barrier semaphores. Data moves between devices by JAX's collectives and lax.ppermute only.
A program may use at most 128 MiB of HBM per device.

```python
import math
import jax
import jax.numpy as jnp
from jax import lax

H = 64
P_SIZE = 64
N = 128
Q = 128
TERMS = 4
LENGTH = 4096
SEQS = 8


def draw_cotangent(key, part):
    first_key = jax.random.fold_in(jax.random.fold_in(key, 11), 0)
    shape_all = (SEQS, LENGTH, H * P_SIZE)
    ramp_pos = 1.0 + 2.0 * jnp.arange(LENGTH, dtype=jnp.float32) / LENGTH
    ramp_seq = 1.0 + 2.0 * jnp.arange(SEQS, dtype=jnp.float32) / SEQS
    scaled = ramp_seq[:, None, None] * ramp_pos[None, :, None] * 0.5
    values = jnp.clip(jax.random.normal(first_key, shape_all, jnp.float32), -5.0, 5.0) * scaled
    return jnp.clip(values, -23.0, 23.0).astype(jnp.bfloat16)


def draw_step_size(key, part):
    first_key, second_key = jax.random.split(jax.random.fold_in(key, 23))
    blocks = LENGTH // Q
    fine = jax.random.uniform(first_key, (SEQS, H, blocks, Q), jnp.float32, -0.7, 0.7)
    coarse = jax.random.uniform(second_key, (SEQS, H, blocks, 1), jnp.float32, -0.5, 0.5)
    return jnp.exp(fine + coarse).reshape(SEQS, H, LENGTH)


def draw_forget(key, part):
    first_key, second_key = jax.random.split(jax.random.fold_in(key, 37))
    spots = jax.random.randint(first_key, (SEQS, 2), 0, LENGTH)
    sizes = jax.random.uniform(second_key, (SEQS, 2), jnp.float32, 0.22, 0.5)
    places = jnp.arange(LENGTH, dtype=jnp.int32)
    hits = (places[None, None, :] == spots[:, :, None]).astype(jnp.float32)
    return jnp.sum(hits * sizes[:, :, None], axis=1)


def draw_decay_rate(key, part):
    first_key = jax.random.fold_in(jax.random.fold_in(key, 41), 0)
    low_end = math.log(0.02 / LENGTH)
    return jnp.exp(jax.random.uniform(first_key, (H,), jnp.float32, low_end, math.log(0.04)))


def steps_of(rng, dims, cuts, low, top_value):
    loudness, own = 1.0, jax.random.fold_in(rng, 6)
    for dim, parts in cuts:
        heights = jnp.exp(jax.random.uniform(jax.random.fold_in(own, dim), (parts,), jnp.float32, low / len(cuts), top_value / len(cuts)))
        loudness = loudness * jnp.repeat(heights, dims[dim] // parts).reshape([-1 if axis == dim else 1 for axis in range(len(dims))])
    return loudness


def noise(key, extent, spread, limit, cuts=(), kind=jnp.bfloat16):
    result = spread * jax.random.normal(key, extent, jnp.float32)
    if cuts:
        result = result * steps_of(key, extent, cuts, -0.22, 0.18)
    return jnp.clip(result, -limit, limit).astype(kind)


def setup_inputs(seed: int = 0) -> dict:
    seeds = jax.random.split(jax.random.key(seed), 9)
    return {
        "cotangent": draw_cotangent(jax.random.fold_in(seeds[8], 71), 0),
        "fixed_point": noise(seeds[1], (SEQS, LENGTH, H * P_SIZE), 1.0, 6.0, ((0, 8), (1, 32))),
        "input_map": noise(seeds[2], (SEQS, LENGTH, N), (4 * N * LENGTH) ** -0.5, 0.00390625, ((0, 8), (1, 32))),
        "output_map": noise(seeds[3], (SEQS, LENGTH, N), 1.0, 6.0, ((0, 8), (1, 32))),
        "step_size": draw_step_size(jax.random.fold_in(seeds[8], 71), 0),
        "forget": draw_forget(jax.random.fold_in(seeds[8], 71), 0),
        "decay_rate": draw_decay_rate(jax.random.fold_in(seeds[8], 71), 0),
        "skip_gain": jnp.clip(jax.random.uniform(seeds[7], (H,), jnp.float32, 0.3, 0.65), 0.3, 0.65),
    }


HIGHEST_PRECISION = lax.Precision.HIGHEST


def tables(input_rows, output_rows, step_rows, forget, decay_rate):
    log_step = -decay_rate[:, None, None] * step_rows - forget[None, :, :]
    log_decay = jnp.cumsum(log_step, axis=2)
    step_sum = jnp.cumsum(step_rows, axis=2)
    decay_end = log_decay[:, :, -1]
    block_len = log_decay.shape[2]
    causal = lax.broadcasted_iota(jnp.int32, (block_len, block_len), 0) >= lax.broadcasted_iota(jnp.int32, (block_len, block_len), 1)
    scores = jnp.einsum('ktn,ksn->kts', output_rows.astype(jnp.float32), input_rows.astype(jnp.float32))
    log_gap = jnp.where(causal[None, None], log_decay[:, :, :, None] - log_decay[:, :, None, :], -jnp.inf)
    mixing = (scores[None] * jnp.exp(log_gap) * step_rows[:, :, None, :]).astype(jnp.bfloat16)
    input_weight = ((step_rows * jnp.exp(decay_end[:, :, None] - log_decay))[..., None] * input_rows[None].astype(jnp.float32)).astype(jnp.bfloat16)
    output_weight = (jnp.exp(log_decay)[..., None] * output_rows[None].astype(jnp.float32)).astype(jnp.bfloat16)
    mixing, input_weight, output_weight = lax.optimization_barrier((mixing, input_weight, output_weight))
    decay_run = jnp.cumsum(decay_end, axis=1)
    blocks = decay_end.shape[1]
    rows_at = lax.broadcasted_iota(jnp.int32, (blocks, blocks), 0)
    cols_at = lax.broadcasted_iota(jnp.int32, (blocks, blocks), 1)
    back_reach = jnp.exp(jnp.where((cols_at > rows_at)[None], decay_run[:, None, :] - decay_end[:, None, :] - decay_run[:, :, None], -jnp.inf))
    fore_reach = jnp.exp(jnp.where((cols_at < rows_at)[None], decay_run[:, :, None] - decay_end[:, :, None] - decay_run[:, None, :], -jnp.inf))
    return mixing, input_weight, output_weight, decay_end, decay_run, step_sum, back_reach, fore_reach


def rounded_wide(values):
    narrow = lax.optimization_barrier(values.astype(jnp.bfloat16))
    return narrow.astype(jnp.float32)


def forward_apply(group_table, fixed_wide):
    state_local = jnp.einsum('hksn,kshp->hknp', group_table[1].astype(jnp.float32), fixed_wide)
    state_in = jnp.einsum('hkj,hjnp->hknp', group_table[7], state_local, precision=HIGHEST_PRECISION)
    outputs = jnp.einsum('hkts,kshp->kthp', group_table[0].astype(jnp.float32), fixed_wide)
    outputs = outputs + jnp.einsum('hktn,hknp->kthp', group_table[2].astype(jnp.float32), rounded_wide(state_in))
    state_out = state_local + jnp.exp(group_table[3])[..., None, None] * state_in
    return outputs, state_out


def backward_apply(group_table, vector_wide):
    state_local = jnp.einsum('hktn,kthp->hknp', group_table[2].astype(jnp.float32), vector_wide)
    state_in = jnp.einsum('hkj,hjnp->hknp', group_table[6], state_local, precision=HIGHEST_PRECISION)
    adjoint = jnp.einsum('hkts,kthp->kshp', group_table[0].astype(jnp.float32), vector_wide)
    adjoint = adjoint + jnp.einsum('hksn,hknp->kshp', group_table[1].astype(jnp.float32), rounded_wide(state_in))
    return adjoint, state_in


def pieces(step_sum, vector_wide, fixed_wide, outputs, adjoint, state_out, state_in):
    skip_part = jnp.sum(vector_wide * fixed_wide, axis=(0, 1, 3))
    step_rows = jnp.transpose(step_sum, (1, 2, 0))[..., None]
    inner_sum = jnp.sum(step_rows * (vector_wide * outputs - fixed_wide * adjoint), axis=(0, 1, 3))
    third_sum = jnp.sum(step_sum[:, :, -1][:, :, None, None] * state_out * state_in, axis=(1, 2, 3))
    return -(inner_sum + third_sum), skip_part


def one_sequence(cotangent, fixed_point, input_map, output_map, step_size, forget, decay_rate, skip_gain):
    groups = LENGTH // Q
    group_shape = (groups, Q, H, P_SIZE)
    vector = cotangent.reshape(group_shape)
    fixed_wide = fixed_point.reshape(group_shape).astype(jnp.float32)
    group_table = tables(input_map.reshape(groups, Q, N), output_map.reshape(groups, Q, N), step_size.reshape(H, groups, Q), forget.reshape(groups, Q), decay_rate)
    outputs, state_out = forward_apply(group_table, fixed_wide)
    summed = jnp.zeros(group_shape, jnp.float32)
    rate_sum = jnp.zeros((H,), jnp.float32)
    skip_sum = jnp.zeros((H,), jnp.float32)
    for number in range(TERMS):
        vector_wide = vector.astype(jnp.float32)
        adjoint, state_in = backward_apply(group_table, vector_wide)
        rate_part, skip_part = pieces(group_table[5], vector_wide, fixed_wide, outputs, adjoint, state_out, state_in)
        rate_sum = rate_sum + rate_part
        skip_sum = skip_sum + skip_part
        summed = summed + vector_wide
        if number + 1 < TERMS:
            vector = lax.optimization_barrier((adjoint + skip_gain[None, None, :, None] * vector_wide).astype(jnp.bfloat16))
    return summed.astype(jnp.bfloat16).reshape(LENGTH, H * P_SIZE), rate_sum, skip_sum


def reference(cotangent, fixed_point, input_map, output_map, step_size, forget, decay_rate, skip_gain):
    def run(members):
        return one_sequence(*members, decay_rate, skip_gain)

    adjoint_sum, rate_parts, skip_parts = lax.map(run, (cotangent, fixed_point, input_map, output_map, step_size, forget))
    divisor = jnp.float32(SEQS * LENGTH)
    return adjoint_sum, jnp.sum(rate_parts, axis=0) / divisor, jnp.sum(skip_parts, axis=0) / divisor
```

```python
import jax
import jax.numpy as jnp
from jax import lax
from jax.experimental import pallas as pl
from jax.experimental.pallas import tpu as pltpu
from jax.sharding import Mesh
from jax.sharding import PartitionSpec as P

H = 64
HEAD = 64
N = 128
Q = 128
EXTRA = 8
GROUPS = 32
NY = 4
NZ = 8
UNROLL = 4
SEQ = ("seq_0", "seq_1")
BATCH = ("batch_0", "batch_1")
F32 = jnp.float32
BF16 = jnp.bfloat16


def shifted(x, axis, by):
    size = lax.axis_size(axis)
    return lax.ppermute(x, axis, [(i, (i + by) % size) for i in range(size)])


def swapped(x, axis, bit):
    size = lax.axis_size(axis)
    return lax.ppermute(x, axis, [(i, i ^ bit) for i in range(size)])


def halves(x):
    high = x.astype(BF16)
    return high, (x - high.astype(F32)).astype(BF16)


def pack_kernel(cot_ref, step_ref, forget_ref, out_ref):
    step_high, step_low = halves(step_ref[...])
    forget_high, forget_low = halves(forget_ref[...])
    for j in range(4):
        out_ref[j, :Q, :] = cot_ref[:, j * 128 : (j + 1) * 128]
        rows = jnp.concatenate(
            [
                step_high[2 * j : 2 * j + 2].astype(F32),
                step_low[2 * j : 2 * j + 2].astype(F32),
                forget_high.astype(F32),
                forget_low.astype(F32),
                jnp.zeros((2, Q), F32),
            ],
            axis=0,
        )
        out_ref[j, Q : Q + EXTRA, :] = rows.astype(BF16)


def pack(cot, step, forget):
    return pl.pallas_call(
        pack_kernel,
        grid=(8,),
        in_specs=[
            pl.BlockSpec((Q, 512), lambda i: (0, i)),
            pl.BlockSpec((8, Q), lambda i: (i, 0)),
            pl.BlockSpec((1, Q), lambda i: (0, 0)),
        ],
        out_specs=pl.BlockSpec((4, Q + EXTRA, 128), lambda i: (i, 0, 0)),
        out_shape=jax.ShapeDtypeStruct((GROUPS, Q + EXTRA, 128), BF16),
        name="pack",
    )(cot, step, forget)


def split_kernel(in_ref, out_ref):
    for j in range(4):
        out_ref[j] = in_ref[:, j * 128 : (j + 1) * 128]


def split(x):
    return pl.pallas_call(
        split_kernel,
        grid=(8,),
        in_specs=[pl.BlockSpec((Q, 512), lambda i: (0, i))],
        out_specs=pl.BlockSpec((4, Q, 128), lambda i: (i, 0, 0)),
        out_shape=jax.ShapeDtypeStruct((GROUPS, Q, 128), BF16),
        name="split",
    )(x)


def join_kernel(in_ref, out_ref):
    for j in range(4):
        out_ref[:, j * 128 : (j + 1) * 128] = in_ref[j]


def join(x):
    return pl.pallas_call(
        join_kernel,
        grid=(8,),
        in_specs=[pl.BlockSpec((4, Q, 128), lambda i: (i, 0, 0))],
        out_specs=pl.BlockSpec((Q, 512), lambda i: (0, i)),
        out_shape=jax.ShapeDtypeStruct((Q, GROUPS * 128), BF16),
        name="join",
    )(x)


def dot(a, b):
    return lax.dot_general(a, b, (((1,), (0,)), ((), ())), preferred_element_type=F32)


def dot_t(a, b):
    return lax.dot_general(a, b, (((1,), (1,)), ((), ())), preferred_element_type=F32)


def fetch_maps(pos_ref, pieces, maps_ref, sem):
    my_y, my_z = pos_ref[0], pos_ref[1]
    copies = []
    for dy in range(NY):
        for dz in range(NZ):
            if dy == 0:
                source = pieces[0].at[dz]
            elif dy == 1:
                source = pieces[1].at[dz]
            elif dy == 3:
                source = pieces[2].at[dz]
            else:
                source = pieces[3].at[dz] if dz < 4 else pieces[4].at[dz - 4]
            place = ((my_y + dy) % NY) * NZ + (my_z + dz) % NZ
            copies.append(pltpu.make_async_copy(source, maps_ref.at[place], sem))
    for c in copies:
        c.start()
    for c in copies:
        c.wait()


def constants():
    rows = lax.broadcasted_iota(jnp.int32, (Q, Q), 0)
    cols = lax.broadcasted_iota(jnp.int32, (Q, Q), 1)
    lower = (rows >= cols).astype(F32).astype(BF16)
    same = (rows == cols).astype(F32).astype(BF16)
    return rows <= cols, lower, same


def prepare(c, in_ref, maps_ref, rate_ref, consts, mat_ref, turn_ref, e_ref, g_ref, s_ref, m_ref):
    upper, lower, same = consts
    both = maps_ref[c]
    b_rows, c_rows = both[:N], both[N:]
    prod = dot_t(jnp.concatenate([b_rows, same], axis=0), c_rows)
    mat_ref[c, :, :N] = jnp.where(upper, prod[:Q], 0.0).astype(BF16)
    mat_ref[c, :, N:] = b_rows
    turn_ref[c] = prod[Q:].astype(BF16)
    rows = in_ref[c, Q : Q + EXTRA, :].astype(F32)

    def wide(first, second):
        return jnp.concatenate(
            [jnp.broadcast_to(rows[first : first + 1], (HEAD, Q)), jnp.broadcast_to(rows[second : second + 1], (HEAD, Q))],
            axis=0,
        ).astype(BF16)

    steps = jnp.concatenate([wide(0, 1), wide(2, 3)], axis=1)
    forgets = jnp.concatenate([wide(4, 4), wide(5, 5)], axis=1)
    lower_twice = jnp.concatenate([lower, lower], axis=1)
    same_twice = jnp.concatenate([same, same], axis=1)
    sums = dot_t(jnp.concatenate([lower_twice, same_twice], axis=0), steps)
    step_sum, step_col = sums[:Q], sums[Q:]
    forget_sum = dot_t(lower_twice, forgets)
    log_decay = -(rate_ref[0:1, :] * step_sum + forget_sum)
    middle = 0.5 * log_decay[Q - 1 : Q, :]
    gap = log_decay - middle
    e_ref[c] = jnp.exp(gap)
    g_ref[c] = step_col * jnp.exp(-gap)
    if s_ref is not None:
        s_ref[c] = step_sum
    m_ref[c] = jnp.broadcast_to(jnp.exp(middle), (8, 128))


def series_kernel(pos_ref, in_ref, p0, p1, p2, p3, p4, rate_ref, out_ref, maps_ref, mat_ref, turn_ref, e_ref, g_ref, m_ref, v_ref, sum_ref, back_ref, sem):
    fetch_maps(pos_ref, (p0, p1, p2, p3, p4), maps_ref, sem)
    consts = constants()

    def prep(i, _):
        for j in range(2):
            prepare(i * 2 + j, in_ref, maps_ref, rate_ref, consts, mat_ref, turn_ref, e_ref, g_ref, None, m_ref)
        return 0

    lax.fori_loop(0, GROUPS // 2, prep, 0)
    skip = rate_ref[1:2, :]
    for k in range(3):
        back_ref[...] = jnp.zeros((N, 128), F32)

        def step(i, _):
            back = back_ref[...]
            for j in range(UNROLL):
                c = GROUPS - 1 - (i * UNROLL + j)
                v = (in_ref[c, :Q, :] if k == 0 else v_ref[c]).astype(F32)
                x = (e_ref[c] * v).astype(BF16)
                local = dot(turn_ref[c], x)
                adj = g_ref[c] * dot(mat_ref[c], jnp.concatenate([x, back.astype(BF16)], axis=0))
                scale = m_ref[c, 0:1, :] * m_ref[jnp.maximum(c - 1, 0), 0:1, :]
                back = scale * (back + local)
                new = (adj + skip * v).astype(BF16)
                total = (v if k == 0 else sum_ref[c]) + new.astype(F32)
                if k < 2:
                    v_ref[c] = new
                    sum_ref[c] = total
                else:
                    out_ref[c] = total.astype(BF16)
            back_ref[...] = back
            return 0

        lax.fori_loop(0, GROUPS // UNROLL, step, 0)


def rate_kernel(pos_ref, in_ref, sum_ref, fixed_ref, p0, p1, p2, p3, p4, rate_ref, out_ref, maps_ref, mat_ref, turn_ref, e_ref, g_ref, s_ref, m_ref, back_ref, acc_ref, sem):
    fetch_maps(pos_ref, (p0, p1, p2, p3, p4), maps_ref, sem)
    consts = constants()

    def prep(i, _):
        for j in range(2):
            prepare(i * 2 + j, in_ref, maps_ref, rate_ref, consts, mat_ref, turn_ref, e_ref, g_ref, s_ref, m_ref)
        return 0

    lax.fori_loop(0, GROUPS // 2, prep, 0)
    back_ref[...] = jnp.zeros((N, 256), F32)
    acc_ref[...] = jnp.zeros((2, 8, 128), F32)

    def step(i, _):
        back, tangent = back_ref[:, :128], back_ref[:, 128:]
        rate_sum, skip_sum = acc_ref[0], acc_ref[1]
        for j in range(2):
            c = GROUPS - 1 - (i * 2 + j)
            v = sum_ref[c].astype(F32)
            z = fixed_ref[c].astype(F32)
            s = s_ref[c]
            ev = e_ref[c] * v
            x = jnp.concatenate([ev.astype(BF16), (ev * s).astype(BF16)], axis=1)
            local = dot(turn_ref[c], x)
            tangent = tangent + s[Q - 1 : Q, :] * back
            state = jnp.concatenate([back.astype(BF16), tangent.astype(BF16)], axis=1)
            both = dot(mat_ref[c], jnp.concatenate([x, state], axis=0))
            change = g_ref[c] * (both[:, 128:] - s * both[:, :128])
            rate_sum = rate_sum + jnp.sum((z * change).reshape(16, 8, 128), axis=0)
            skip_sum = skip_sum + jnp.sum((z * v).reshape(16, 8, 128), axis=0)
            scale = m_ref[c, 0:1, :] * m_ref[jnp.maximum(c - 1, 0), 0:1, :]
            back = scale * (back + local[:, :128])
            tangent = scale * (tangent + local[:, 128:])
        back_ref[:, :128] = back
        back_ref[:, 128:] = tangent
        acc_ref[0] = rate_sum
        acc_ref[1] = skip_sum
        return 0

    lax.fori_loop(0, GROUPS // 2, step, 0)
    lane = lax.broadcasted_iota(jnp.int32, (8, 128), 1)
    row = lax.broadcasted_iota(jnp.int32, (8, 128), 0)
    first = (pos_ref[0] * NZ + pos_ref[1]) * 2
    result = jnp.zeros((8, 128), F32)
    for kind in range(2):
        for head in range(2):
            picked = jnp.where((lane >= HEAD) if head else (lane < HEAD), acc_ref[kind], 0.0)
            value = jnp.sum(picked, keepdims=True)
            value = -value if kind == 0 else value
            result = jnp.where((row == kind) & (lane == first + head), value, result)
    out_ref[...] = result


def full(shape):
    return pl.BlockSpec(shape, lambda *_: (0,) * len(shape))


HBM = pl.BlockSpec(memory_space=pltpu.HBM)
SMEM = pl.BlockSpec(memory_space=pltpu.SMEM)


def table_scratch(with_sums):
    square = pltpu.VMEM((GROUPS, Q, 128), F32)
    return [
        pltpu.VMEM((GROUPS, 2 * N, 128), BF16),
        pltpu.VMEM((GROUPS, Q, 256), BF16),
        pltpu.VMEM((GROUPS, N, Q), BF16),
        square,
        square,
        *([square] if with_sums else []),
        pltpu.VMEM((GROUPS, 8, 128), F32),
    ]


def series(pos, rows, pieces, rate):
    return pl.pallas_call(
        series_kernel,
        in_specs=[SMEM, full(rows.shape), HBM, HBM, HBM, HBM, HBM, full(rate.shape)],
        out_specs=full((GROUPS, Q, 128)),
        out_shape=jax.ShapeDtypeStruct((GROUPS, Q, 128), BF16),
        scratch_shapes=[
            *table_scratch(False),
            pltpu.VMEM((GROUPS, Q, 128), BF16),
            pltpu.VMEM((GROUPS, Q, 128), F32),
            pltpu.VMEM((N, 128), F32),
            pltpu.SemaphoreType.DMA,
        ],
        name="series",
        cost_estimate=pl.CostEstimate(flops=3_000_000_000, transcendentals=1_000_000, bytes_accessed=5_000_000),
    )(pos, rows, *pieces, rate)


def rates(pos, rows, summed, fixed, pieces, rate):
    return pl.pallas_call(
        rate_kernel,
        in_specs=[SMEM, full(rows.shape), full(summed.shape), full(fixed.shape), HBM, HBM, HBM, HBM, HBM, full(rate.shape)],
        out_specs=full((8, 128)),
        out_shape=jax.ShapeDtypeStruct((8, 128), F32),
        scratch_shapes=[
            *table_scratch(True),
            pltpu.VMEM((N, 256), F32),
            pltpu.VMEM((2, 8, 128), F32),
            pltpu.SemaphoreType.DMA,
        ],
        name="rates",
        cost_estimate=pl.CostEstimate(flops=2_000_000_000, transcendentals=1_000_000, bytes_accessed=5_000_000),
    )(pos, rows, summed, fixed, *pieces, rate)


def gather_maps(input_map, output_map):
    own = jnp.concatenate([input_map, output_map], axis=0)
    up, down = [own], [own]
    for _ in range(3):
        up.append(shifted(up[-1], "seq_1", 1))
        down.append(shifted(down[-1], "seq_1", -1))
    far_first = shifted(up[3][:N], "seq_1", 1)
    far_second = shifted(down[3][N:], "seq_1", -1)
    far = jnp.concatenate([far_first, far_second], axis=0)
    line = jnp.stack([own, down[1], down[2], down[3], far, up[3], up[2], up[1]])
    from_next = shifted(line, "seq_0", -1)
    from_last = shifted(line, "seq_0", 1)
    low = shifted(from_last[:4], "seq_0", 1)
    high = shifted(from_next[4:], "seq_0", -1)
    return line, from_next, from_last, low, high


def body(cotangent, fixed_point, input_map, output_map, step_size, forget, decay_rate, skip_gain):
    my_y, my_z = lax.axis_index("seq_0"), lax.axis_index("seq_1")
    pos = jnp.stack([my_y, my_z]).astype(jnp.int32)
    first = (my_y * NZ + my_z) * 2
    own = jnp.stack([lax.dynamic_slice_in_dim(a, first, 2) for a in (decay_rate, skip_gain)])
    rate = jnp.repeat(own, HEAD, axis=1)

    packed = pack(cotangent[0], step_size[0], forget)
    rows = lax.all_to_all(packed, SEQ, split_axis=0, concat_axis=0, tiled=True)
    pieces = gather_maps(input_map[0], output_map[0])
    fixed = lax.all_to_all(split(fixed_point[0]), SEQ, split_axis=0, concat_axis=0, tiled=True)
    summed = series(pos, rows, pieces, rate)
    result = lax.all_to_all(summed, SEQ, split_axis=0, concat_axis=0, tiled=True)
    totals = rates(pos, rows, summed, fixed, pieces, rate)
    for axis in ("batch_1", "batch_0", "seq_0", "seq_1"):
        bit = 1
        while bit < lax.axis_size(axis):
            totals = totals + swapped(totals, axis, bit)
            bit *= 2
    scale = 1.0 / (lax.axis_size(BATCH) * Q * GROUPS)
    return join(result)[None], totals[0, :H] * scale, totals[1, :H] * scale


def solution(mesh):
    torus = Mesh(mesh.devices.reshape(4, 2, 4, 8), ("batch_0", "batch_1", "seq_0", "seq_1"))
    return jax.shard_map(
        body,
        mesh=torus,
        in_specs=(
            P(BATCH, SEQ, None),
            P(BATCH, SEQ, None),
            P(BATCH, SEQ, None),
            P(BATCH, SEQ, None),
            P(BATCH, None, SEQ),
            P(BATCH, SEQ),
            P(),
            P(),
        ),
        out_specs=(P(BATCH, SEQ, None), P(), P()),
        check_vma=False,
    )
```

```python
import jax
import jax.numpy as jnp
from jax import lax
from jax.experimental import pallas as pl
from jax.experimental.pallas import tpu as pltpu
from jax.sharding import Mesh
from jax.sharding import PartitionSpec as P

H = 64
HEAD = 64
N = 128
Q = 128
EXTRA = 8
GROUPS = 32
NY = 4
NZ = 8
UNROLL = 16
PREP = 16
PAIRED = 8
SEQ = ("seq_0", "seq_1")
BATCH = ("batch_0", "batch_1")
F32 = jnp.float32
BF16 = jnp.bfloat16


def shifted(x, axis, by):
    size = lax.axis_size(axis)
    return lax.ppermute(x, axis, [(i, (i + by) % size) for i in range(size)])


def swapped(x, axis, bit):
    size = lax.axis_size(axis)
    return lax.ppermute(x, axis, [(i, i ^ bit) for i in range(size)])


def full(shape):
    return pl.BlockSpec(shape, lambda *_: (0,) * len(shape))


HBM = pl.BlockSpec(memory_space=pltpu.HBM)
SMEM = pl.BlockSpec(memory_space=pltpu.SMEM)


def halves(x):
    high = x.astype(BF16)
    return high, (x - high.astype(F32)).astype(BF16)


def pack_kernel(step_ref, forget_ref, cot_ref, out_ref, sem):
    copies = [
        pltpu.make_async_copy(cot_ref.at[:, pl.ds(j * 128, 128)], out_ref.at[j, pl.ds(0, Q), :], sem)
        for j in range(GROUPS)
    ]
    for c in copies:
        c.start()
    step_high, step_low = halves(step_ref[...])
    step_high, step_low = step_high.astype(F32), step_low.astype(F32)
    tail = [f.astype(F32) for f in halves(forget_ref[...])] + [jnp.zeros((2, Q), F32)]
    for j in range(GROUPS):
        two = slice(2 * j, 2 * j + 2)
        rows = jnp.concatenate([step_high[two], step_low[two], *tail], axis=0)
        out_ref[j, Q : Q + EXTRA, :] = rows.astype(BF16)
    for c in copies:
        c.wait()


def pack(cot, step, forget):
    return pl.pallas_call(
        pack_kernel,
        in_specs=[full(step.shape), full(forget.shape), HBM],
        out_specs=full((GROUPS, Q + EXTRA, 128)),
        out_shape=jax.ShapeDtypeStruct((GROUPS, Q + EXTRA, 128), BF16),
        scratch_shapes=[pltpu.SemaphoreType.DMA],
        name="pack",
    )(step, forget, cot)


def split_kernel(in_ref, out_ref, sem):
    copies = [
        pltpu.make_async_copy(in_ref.at[:, pl.ds(j * 128, 128)], out_ref.at[j], sem) for j in range(GROUPS)
    ]
    for c in copies:
        c.start()
    for c in copies:
        c.wait()


def split(x):
    return pl.pallas_call(
        split_kernel,
        in_specs=[HBM],
        out_specs=full((GROUPS, Q, 128)),
        out_shape=jax.ShapeDtypeStruct((GROUPS, Q, 128), BF16),
        scratch_shapes=[pltpu.SemaphoreType.DMA],
        name="split",
    )(x)


def join_kernel(in_ref, out_ref, sem):
    copies = [
        pltpu.make_async_copy(in_ref.at[j], out_ref.at[:, pl.ds(j * 128, 128)], sem) for j in range(GROUPS)
    ]
    for c in copies:
        c.start()
    for c in copies:
        c.wait()


def join(x):
    return pl.pallas_call(
        join_kernel,
        in_specs=[full(x.shape)],
        out_specs=HBM,
        out_shape=jax.ShapeDtypeStruct((Q, GROUPS * 128), BF16),
        scratch_shapes=[pltpu.SemaphoreType.DMA],
        name="join",
    )(x)


def dot(a, b):
    return lax.dot_general(a, b, (((1,), (0,)), ((), ())), preferred_element_type=F32)


def dot_t(a, b):
    return lax.dot_general(a, b, (((1,), (1,)), ((), ())), preferred_element_type=F32)


def fetch_maps(pos_ref, pieces, maps_ref, sem):
    my_y, my_z = pos_ref[0], pos_ref[1]
    copies = []
    for dy in range(NY):
        for dz in range(NZ):
            if dy == 0:
                source = pieces[0].at[dz]
            elif dy == 1:
                source = pieces[1].at[dz]
            elif dy == 3:
                source = pieces[2].at[dz]
            else:
                source = pieces[3].at[dz] if dz < 4 else pieces[4].at[dz - 4]
            place = ((my_y + dy) % NY) * NZ + (my_z + dz) % NZ
            copies.append(pltpu.make_async_copy(source, maps_ref.at[place], sem))
    for c in copies:
        c.start()
    for c in copies:
        c.wait()


def constants():
    rows = lax.broadcasted_iota(jnp.int32, (Q, Q), 0)
    cols = lax.broadcasted_iota(jnp.int32, (Q, Q), 1)
    lower = (rows >= cols).astype(F32).astype(BF16)
    same = (rows == cols).astype(F32).astype(BF16)
    return rows <= cols, lower, same


def prepare(c, in_ref, maps_ref, rate_ref, consts, mat_ref, turn_ref, e_ref, g_ref, s_ref, m_ref):
    upper, lower, same = consts
    both = maps_ref[c]
    b_rows, c_rows = both[:N], both[N:]
    prod = dot_t(jnp.concatenate([b_rows, same], axis=0), c_rows)
    mat_ref[c, :, :N] = jnp.where(upper, prod[:Q], 0.0).astype(BF16)
    mat_ref[c, :, N:] = b_rows
    turn_ref[c] = prod[Q:].astype(BF16)
    rows = in_ref[c, Q : Q + EXTRA, :].astype(F32)

    def wide(first, second):
        return jnp.concatenate(
            [jnp.broadcast_to(rows[first : first + 1], (HEAD, Q)), jnp.broadcast_to(rows[second : second + 1], (HEAD, Q))],
            axis=0,
        ).astype(BF16)

    steps = jnp.concatenate([wide(0, 1), wide(2, 3)], axis=1)
    forgets = jnp.concatenate([wide(4, 4), wide(5, 5)], axis=1)
    lower_twice = jnp.concatenate([lower, lower], axis=1)
    same_twice = jnp.concatenate([same, same], axis=1)
    sums = dot_t(jnp.concatenate([lower_twice, same_twice], axis=0), steps)
    step_sum, step_col = sums[:Q], sums[Q:]
    forget_sum = dot_t(lower_twice, forgets)
    log_decay = -(rate_ref[0:1, :] * step_sum + forget_sum)
    middle = 0.5 * log_decay[Q - 1 : Q, :]
    gap = log_decay - middle
    e_ref[c] = jnp.exp(gap)
    g_ref[c] = step_col * jnp.exp(-gap)
    if s_ref is not None:
        s_ref[c] = step_sum
    m_ref[c] = jnp.broadcast_to(jnp.exp(middle), (8, 128))


def series_kernel(pos_ref, in_ref, p0, p1, p2, p3, p4, rate_ref, out_ref, maps_ref, mat_ref, turn_ref, e_ref, g_ref, m_ref, v_ref, sum_ref, back_ref, sem):
    fetch_maps(pos_ref, (p0, p1, p2, p3, p4), maps_ref, sem)
    consts = constants()

    def prep(i, _):
        for j in range(PREP):
            prepare(i * PREP + j, in_ref, maps_ref, rate_ref, consts, mat_ref, turn_ref, e_ref, g_ref, None, m_ref)
        return 0

    lax.fori_loop(0, GROUPS // PREP, prep, 0)
    skip = rate_ref[1:2, :]
    for k in range(3):
        back_ref[...] = jnp.zeros((N, 128), F32)

        def step(i, _):
            groups = [GROUPS - 1 - (i * UNROLL + j) for j in range(UNROLL)]
            values = [(in_ref[c, :Q, :] if k == 0 else v_ref[c]).astype(F32) for c in groups]
            turned = [(e_ref[c] * v).astype(BF16) for c, v in zip(groups, values)]
            local = [dot(turn_ref[c], x) for c, x in zip(groups, turned)]
            back = back_ref[...]
            states = []
            for j, c in enumerate(groups):
                states.append(back.astype(BF16))
                scale = m_ref[c, 0:1, :] * m_ref[jnp.maximum(c - 1, 0), 0:1, :]
                back = scale * (back + local[j])
            back_ref[...] = back
            mixed = [
                dot(mat_ref[c], jnp.concatenate([x, b], axis=0)) for c, x, b in zip(groups, turned, states)
            ]
            fresh = [
                (g_ref[c] * r + skip * v).astype(BF16) for c, r, v in zip(groups, mixed, values)
            ]
            totals = [
                (v if k == 0 else sum_ref[c]) + n.astype(F32) for c, v, n in zip(groups, values, fresh)
            ]
            for c, n, t in zip(groups, fresh, totals):
                if k < 2:
                    v_ref[c] = n
                    sum_ref[c] = t
                else:
                    out_ref[c] = t.astype(BF16)
            return 0

        lax.fori_loop(0, GROUPS // UNROLL, step, 0)


def rate_kernel(pos_ref, in_ref, sum_ref, fixed_ref, p0, p1, p2, p3, p4, rate_ref, out_ref, maps_ref, mat_ref, turn_ref, e_ref, g_ref, s_ref, m_ref, back_ref, acc_ref, sem):
    fetch_maps(pos_ref, (p0, p1, p2, p3, p4), maps_ref, sem)
    consts = constants()

    def prep(i, _):
        for j in range(PREP):
            prepare(i * PREP + j, in_ref, maps_ref, rate_ref, consts, mat_ref, turn_ref, e_ref, g_ref, s_ref, m_ref)
        return 0

    lax.fori_loop(0, GROUPS // PREP, prep, 0)
    back_ref[...] = jnp.zeros((N, 256), F32)
    acc_ref[...] = jnp.zeros((2, 8, 128), F32)

    def step(i, _):
        groups = [GROUPS - 1 - (i * PAIRED + j) for j in range(PAIRED)]
        values = [sum_ref[c].astype(F32) for c in groups]
        turned = []
        for c, v in zip(groups, values):
            ev = e_ref[c] * v
            turned.append(jnp.concatenate([ev.astype(BF16), (ev * s_ref[c]).astype(BF16)], axis=1))
        local = [dot(turn_ref[c], x) for c, x in zip(groups, turned)]
        back, tangent = back_ref[:, :128], back_ref[:, 128:]
        states = []
        for j, c in enumerate(groups):
            tangent = tangent + s_ref[c, Q - 1 : Q, :] * back
            states.append(jnp.concatenate([back.astype(BF16), tangent.astype(BF16)], axis=1))
            scale = m_ref[c, 0:1, :] * m_ref[jnp.maximum(c - 1, 0), 0:1, :]
            back = scale * (back + local[j][:, :128])
            tangent = scale * (tangent + local[j][:, 128:])
        back_ref[:, :128] = back
        back_ref[:, 128:] = tangent
        mixed = [dot(mat_ref[c], jnp.concatenate([x, b], axis=0)) for c, x, b in zip(groups, turned, states)]
        rate_sum, skip_sum = acc_ref[0], acc_ref[1]
        for c, v, r in zip(groups, values, mixed):
            z = fixed_ref[c].astype(F32)
            change = g_ref[c] * (r[:, 128:] - s_ref[c] * r[:, :128])
            rate_sum = rate_sum + jnp.sum((z * change).reshape(16, 8, 128), axis=0)
            skip_sum = skip_sum + jnp.sum((z * v).reshape(16, 8, 128), axis=0)
        acc_ref[0] = rate_sum
        acc_ref[1] = skip_sum
        return 0

    lax.fori_loop(0, GROUPS // PAIRED, step, 0)
    lane = lax.broadcasted_iota(jnp.int32, (8, 128), 1)
    first = (pos_ref[0] * NZ + pos_ref[1]) * 2
    result = jnp.zeros((8, 128), F32)
    for kind in range(2):
        for head in range(2):
            picked = jnp.where((lane >= HEAD) if head else (lane < HEAD), acc_ref[kind], 0.0)
            value = jnp.sum(picked, keepdims=True)
            value = -value if kind == 0 else value
            result = jnp.where(lane == kind * H + first + head, value, result)
    out_ref[...] = result


def table_scratch(with_sums):
    square = pltpu.VMEM((GROUPS, Q, 128), F32)
    return [
        pltpu.VMEM((GROUPS, 2 * N, 128), BF16),
        pltpu.VMEM((GROUPS, Q, 256), BF16),
        pltpu.VMEM((GROUPS, N, Q), BF16),
        square,
        square,
        *([square] if with_sums else []),
        pltpu.VMEM((GROUPS, 8, 128), F32),
    ]


def series(pos, rows, pieces, rate):
    return pl.pallas_call(
        series_kernel,
        in_specs=[SMEM, full(rows.shape), HBM, HBM, HBM, HBM, HBM, full(rate.shape)],
        out_specs=full((GROUPS, Q, 128)),
        out_shape=jax.ShapeDtypeStruct((GROUPS, Q, 128), BF16),
        scratch_shapes=[
            *table_scratch(False),
            pltpu.VMEM((GROUPS, Q, 128), BF16),
            pltpu.VMEM((GROUPS, Q, 128), F32),
            pltpu.VMEM((N, 128), F32),
            pltpu.SemaphoreType.DMA,
        ],
        name="series",
        cost_estimate=pl.CostEstimate(flops=3_000_000_000, transcendentals=1_000_000, bytes_accessed=5_000_000),
    )(pos, rows, *pieces, rate)


def rates(pos, rows, summed, fixed, pieces, rate):
    return pl.pallas_call(
        rate_kernel,
        in_specs=[SMEM, full(rows.shape), full(summed.shape), full(fixed.shape), HBM, HBM, HBM, HBM, HBM, full(rate.shape)],
        out_specs=full((8, 128)),
        out_shape=jax.ShapeDtypeStruct((8, 128), F32),
        scratch_shapes=[
            *table_scratch(True),
            pltpu.VMEM((N, 256), F32),
            pltpu.VMEM((2, 8, 128), F32),
            pltpu.SemaphoreType.DMA,
        ],
        name="rates",
        cost_estimate=pl.CostEstimate(flops=2_000_000_000, transcendentals=1_000_000, bytes_accessed=5_000_000),
    )(pos, rows, summed, fixed, *pieces, rate)


def gather_line(input_map, output_map):
    own = jnp.concatenate([input_map, output_map], axis=0)
    up, down = [own], [own]
    for _ in range(3):
        up.append(shifted(up[-1], "seq_1", 1))
        down.append(shifted(down[-1], "seq_1", -1))
    far_first = shifted(up[3][:N], "seq_1", 1)
    far_second = shifted(down[3][N:], "seq_1", -1)
    far = jnp.concatenate([far_first, far_second], axis=0)
    return jnp.stack([own, down[1], down[2], down[3], far, up[3], up[2], up[1]])


def gather_plane(line):
    from_next = shifted(line, "seq_0", -1)
    from_last = shifted(line, "seq_0", 1)
    low = shifted(from_last[:4], "seq_0", 1)
    high = shifted(from_next[4:], "seq_0", -1)
    return line, from_next, from_last, low, high


def inner(cotangent, fixed_point, input_map, output_map, step_size, forget, decay_rate, skip_gain):
    my_y, my_z = lax.axis_index("seq_0"), lax.axis_index("seq_1")
    pos = jnp.stack([my_y, my_z]).astype(jnp.int32)
    first = (my_y * NZ + my_z) * 2
    own = jnp.stack([lax.dynamic_slice_in_dim(a, first, 2) for a in (decay_rate, skip_gain)])
    rate = jnp.repeat(own, HEAD, axis=1)

    line = gather_line(input_map[0], output_map[0])
    packed, line = lax.optimization_barrier((pack(cotangent[0], step_size[0], forget), line))
    pieces = gather_plane(line)
    rows = lax.all_to_all(packed, SEQ, split_axis=0, concat_axis=0, tiled=True)
    fixed = lax.all_to_all(split(fixed_point[0]), SEQ, split_axis=0, concat_axis=0, tiled=True)
    summed = series(pos, rows, pieces, rate)
    result = lax.all_to_all(summed, SEQ, split_axis=0, concat_axis=0, tiled=True)
    totals = rates(pos, rows, summed, fixed, pieces, rate)
    for axis in BATCH:
        bit = 1
        while bit < lax.axis_size(axis):
            totals = totals + swapped(totals, axis, bit)
            bit *= 2
    copies = jnp.broadcast_to(totals[:1], (GROUPS, 1, 128))
    totals = lax.all_to_all(copies, SEQ, split_axis=0, concat_axis=0, tiled=True)
    totals = jnp.sum(totals, axis=(0, 1)) * (1.0 / (lax.axis_size(BATCH) * Q * GROUPS))
    return join(result)[None], totals[:H], totals[H:]


def solution(mesh):
    torus = Mesh(mesh.devices.reshape(4, 2, 4, 8), ("batch_0", "batch_1", "seq_0", "seq_1"))
    return jax.shard_map(
        inner,
        mesh=torus,
        in_specs=(
            P(BATCH, SEQ, None),
            P(BATCH, SEQ, None),
            P(BATCH, SEQ, None),
            P(BATCH, SEQ, None),
            P(BATCH, None, SEQ),
            P(BATCH, SEQ),
            P(),
            P(),
        ),
        out_specs=(P(BATCH, SEQ, None), P(), P()),
        check_vma=False,
    )
```

```python
import jax
import jax.numpy as jnp
from jax import lax
from jax.experimental import pallas as pl
from jax.experimental.pallas import tpu as pltpu
from jax.sharding import Mesh
from jax.sharding import PartitionSpec as P

H = 64
HEAD = 64
N = 128
Q = 128
EXTRA = 8
GROUPS = 32
NY = 4
NZ = 8
UNROLL = 16
PREP = 16
PAIRED = 8
SEQ = ("seq_0", "seq_1")
BATCH = ("batch_0", "batch_1")
F32 = jnp.float32
BF16 = jnp.bfloat16


def shifted(x, axis, by):
    size = lax.axis_size(axis)
    return lax.ppermute(x, axis, [(i, (i + by) % size) for i in range(size)])


def swapped(x, axis, bit):
    size = lax.axis_size(axis)
    return lax.ppermute(x, axis, [(i, i ^ bit) for i in range(size)])


def full(shape):
    return pl.BlockSpec(shape, lambda *_: (0,) * len(shape))


HBM = pl.BlockSpec(memory_space=pltpu.HBM)
SMEM = pl.BlockSpec(memory_space=pltpu.SMEM)


def halves(x):
    high = x.astype(BF16)
    return high, (x - high.astype(F32)).astype(BF16)


def pack_kernel(step_ref, forget_ref, cot_ref, out_ref, sem):
    copies = [
        pltpu.make_async_copy(cot_ref.at[:, pl.ds(j * 128, 128)], out_ref.at[j, pl.ds(0, Q), :], sem)
        for j in range(GROUPS)
    ]
    for c in copies:
        c.start()
    step_high, step_low = halves(step_ref[...])
    step_high, step_low = step_high.astype(F32), step_low.astype(F32)
    tail = [f.astype(F32) for f in halves(forget_ref[...])] + [jnp.zeros((2, Q), F32)]
    for j in range(GROUPS):
        two = slice(2 * j, 2 * j + 2)
        rows = jnp.concatenate([step_high[two], step_low[two], *tail], axis=0)
        out_ref[j, Q : Q + EXTRA, :] = rows.astype(BF16)
    for c in copies:
        c.wait()


def pack(cot, step, forget):
    return pl.pallas_call(
        pack_kernel,
        in_specs=[full(step.shape), full(forget.shape), HBM],
        out_specs=full((GROUPS, Q + EXTRA, 128)),
        out_shape=jax.ShapeDtypeStruct((GROUPS, Q + EXTRA, 128), BF16),
        scratch_shapes=[pltpu.SemaphoreType.DMA],
        name="pack",
    )(step, forget, cot)


def split_kernel(pos_ref, in_ref, *refs):
    outs, sem = refs[:NZ], refs[NZ]
    my_y, my_z = pos_ref[0], pos_ref[1]
    copies = []
    for dz in range(NZ):
        for dy in range(NY):
            owner = ((my_y + dy) % NY) * NZ + (my_z + dz) % NZ
            start = pl.multiple_of(owner * 128, 128)
            copies.append(pltpu.make_async_copy(in_ref.at[:, pl.ds(start, 128)], outs[dz].at[dy], sem))
    for c in copies:
        c.start()
    for c in copies:
        c.wait()


def split(pos, x):
    shape = (NY, Q, 128)
    return pl.pallas_call(
        split_kernel,
        in_specs=[SMEM, HBM],
        out_specs=[full(shape)] * NZ,
        out_shape=[jax.ShapeDtypeStruct(shape, BF16)] * NZ,
        scratch_shapes=[pltpu.SemaphoreType.DMA],
        name="split",
    )(pos, x)


def join_kernel(in_ref, out_ref, sem):
    copies = [
        pltpu.make_async_copy(in_ref.at[j], out_ref.at[:, pl.ds(j * 128, 128)], sem) for j in range(GROUPS)
    ]
    for c in copies:
        c.start()
    for c in copies:
        c.wait()


def join(x):
    return pl.pallas_call(
        join_kernel,
        in_specs=[full(x.shape)],
        out_specs=HBM,
        out_shape=jax.ShapeDtypeStruct((Q, GROUPS * 128), BF16),
        scratch_shapes=[pltpu.SemaphoreType.DMA],
        name="join",
    )(x)


def dot(a, b):
    return lax.dot_general(a, b, (((1,), (0,)), ((), ())), preferred_element_type=F32)


def dot_t(a, b):
    return lax.dot_general(a, b, (((1,), (1,)), ((), ())), preferred_element_type=F32)


def fetch_maps(pos_ref, pieces, maps_ref, sem):
    my_y, my_z = pos_ref[0], pos_ref[1]
    copies = []
    for dy in range(NY):
        for dz in range(NZ):
            if dy == 0:
                source = pieces[0].at[dz]
            elif dy == 1:
                source = pieces[1].at[dz]
            elif dy == 3:
                source = pieces[2].at[dz]
            else:
                source = pieces[3].at[dz] if dz < 4 else pieces[4].at[dz - 4]
            place = ((my_y + dy) % NY) * NZ + (my_z + dz) % NZ
            copies.append(pltpu.make_async_copy(source, maps_ref.at[place], sem))
    for c in copies:
        c.start()
    for c in copies:
        c.wait()


def constants():
    rows = lax.broadcasted_iota(jnp.int32, (Q, Q), 0)
    cols = lax.broadcasted_iota(jnp.int32, (Q, Q), 1)
    lower = (rows >= cols).astype(F32).astype(BF16)
    same = (rows == cols).astype(F32).astype(BF16)
    return rows <= cols, lower, same


def prepare(c, in_ref, maps_ref, rate_ref, consts, mat_ref, turn_ref, e_ref, g_ref, s_ref, m_ref):
    upper, lower, same = consts
    both = maps_ref[c]
    b_rows, c_rows = both[:N], both[N:]
    prod = dot_t(jnp.concatenate([b_rows, same], axis=0), c_rows)
    mat_ref[c, :, :N] = jnp.where(upper, prod[:Q], 0.0).astype(BF16)
    mat_ref[c, :, N:] = b_rows
    turn_ref[c] = prod[Q:].astype(BF16)
    rows = in_ref[c, Q : Q + EXTRA, :].astype(F32)

    def wide(first, second):
        return jnp.concatenate(
            [jnp.broadcast_to(rows[first : first + 1], (HEAD, Q)), jnp.broadcast_to(rows[second : second + 1], (HEAD, Q))],
            axis=0,
        ).astype(BF16)

    steps = jnp.concatenate([wide(0, 1), wide(2, 3)], axis=1)
    forgets = jnp.concatenate([wide(4, 4), wide(5, 5)], axis=1)
    lower_twice = jnp.concatenate([lower, lower], axis=1)
    same_twice = jnp.concatenate([same, same], axis=1)
    sums = dot_t(jnp.concatenate([lower_twice, same_twice], axis=0), steps)
    step_sum, step_col = sums[:Q], sums[Q:]
    forget_sum = dot_t(lower_twice, forgets)
    log_decay = -(rate_ref[0:1, :] * step_sum + forget_sum)
    middle = 0.5 * log_decay[Q - 1 : Q, :]
    gap = log_decay - middle
    e_ref[c] = jnp.exp(gap)
    g_ref[c] = step_col * jnp.exp(-gap)
    if s_ref is not None:
        s_ref[c] = step_sum
    m_ref[c] = jnp.broadcast_to(jnp.exp(middle), (8, 128))


def series_kernel(pos_ref, in_ref, p0, p1, p2, p3, p4, rate_ref, out_ref, maps_ref, mat_ref, turn_ref, e_ref, g_ref, m_ref, v_ref, sum_ref, back_ref, sem):
    fetch_maps(pos_ref, (p0, p1, p2, p3, p4), maps_ref, sem)
    consts = constants()

    def prep(i, _):
        for j in range(PREP):
            prepare(i * PREP + j, in_ref, maps_ref, rate_ref, consts, mat_ref, turn_ref, e_ref, g_ref, None, m_ref)
        return 0

    lax.fori_loop(0, GROUPS // PREP, prep, 0)
    skip = rate_ref[1:2, :]
    for k in range(3):
        back_ref[...] = jnp.zeros((N, 128), F32)

        def step(i, _):
            groups = [GROUPS - 1 - (i * UNROLL + j) for j in range(UNROLL)]
            values = [(in_ref[c, :Q, :] if k == 0 else v_ref[c]).astype(F32) for c in groups]
            turned = [(e_ref[c] * v).astype(BF16) for c, v in zip(groups, values)]
            local = [dot(turn_ref[c], x) for c, x in zip(groups, turned)]
            back = back_ref[...]
            states = []
            for j, c in enumerate(groups):
                states.append(back.astype(BF16))
                scale = m_ref[c, 0:1, :] * m_ref[jnp.maximum(c - 1, 0), 0:1, :]
                back = scale * (back + local[j])
            back_ref[...] = back
            mixed = [
                dot(mat_ref[c], jnp.concatenate([x, b], axis=0)) for c, x, b in zip(groups, turned, states)
            ]
            fresh = [
                (g_ref[c] * r + skip * v).astype(BF16) for c, r, v in zip(groups, mixed, values)
            ]
            totals = [
                (v if k == 0 else sum_ref[c]) + n.astype(F32) for c, v, n in zip(groups, values, fresh)
            ]
            for c, n, t in zip(groups, fresh, totals):
                if k < 2:
                    v_ref[c] = n
                    sum_ref[c] = t
                else:
                    out_ref[c] = t.astype(BF16)
            return 0

        lax.fori_loop(0, GROUPS // UNROLL, step, 0)


def tangent_kernel(pos_ref, in_ref, sum_ref, p0, p1, p2, p3, p4, rate_ref, out_ref, maps_ref, mat_ref, turn_ref, e_ref, g_ref, s_ref, m_ref, back_ref, sem):
    fetch_maps(pos_ref, (p0, p1, p2, p3, p4), maps_ref, sem)
    consts = constants()

    def prep(i, _):
        for j in range(PREP):
            prepare(i * PREP + j, in_ref, maps_ref, rate_ref, consts, mat_ref, turn_ref, e_ref, g_ref, s_ref, m_ref)
        return 0

    lax.fori_loop(0, GROUPS // PREP, prep, 0)
    back_ref[...] = jnp.zeros((N, 256), F32)

    def step(i, _):
        groups = [GROUPS - 1 - (i * PAIRED + j) for j in range(PAIRED)]
        values = [sum_ref[c].astype(F32) for c in groups]
        turned = []
        for c, v in zip(groups, values):
            ev = e_ref[c] * v
            turned.append(jnp.concatenate([ev.astype(BF16), (ev * s_ref[c]).astype(BF16)], axis=1))
        local = [dot(turn_ref[c], x) for c, x in zip(groups, turned)]
        back, tangent = back_ref[:, :128], back_ref[:, 128:]
        states = []
        for j, c in enumerate(groups):
            tangent = tangent + s_ref[c, Q - 1 : Q, :] * back
            states.append(jnp.concatenate([back.astype(BF16), tangent.astype(BF16)], axis=1))
            scale = m_ref[c, 0:1, :] * m_ref[jnp.maximum(c - 1, 0), 0:1, :]
            back = scale * (back + local[j][:, :128])
            tangent = scale * (tangent + local[j][:, 128:])
        back_ref[:, :128] = back
        back_ref[:, 128:] = tangent
        mixed = [dot(mat_ref[c], jnp.concatenate([x, b], axis=0)) for c, x, b in zip(groups, turned, states)]
        for c, r in zip(groups, mixed):
            out_ref[c] = g_ref[c] * (s_ref[c] * r[:, :128] - r[:, 128:])
        return 0

    lax.fori_loop(0, GROUPS // PAIRED, step, 0)


def dots_kernel(pos_ref, sum_ref, change_ref, *refs):
    lines, planes = refs[:NZ], refs[NZ : NZ + NY - 1]
    out_ref, fixed_ref, sem = refs[NZ + NY - 1 :]
    my_y, my_z = pos_ref[0], pos_ref[1]
    copies = []
    for dz in range(NZ):
        for dy in range(NY):
            source = lines[dz].at[0] if dy == 0 else planes[dy - 1].at[dz]
            place = ((my_y + NY - dy) % NY) * NZ + (my_z + NZ - dz) % NZ
            copies.append(pltpu.make_async_copy(source, fixed_ref.at[place], sem))
    for c in copies:
        c.start()
    for c in copies:
        c.wait()

    def step(i, sums):
        rate_sum, skip_sum = sums
        for j in range(4):
            c = i * 4 + j
            z = fixed_ref[c].astype(F32)
            v = sum_ref[c].astype(F32)
            rate_sum = rate_sum + jnp.sum((z * change_ref[c]).reshape(16, 8, 128), axis=0)
            skip_sum = skip_sum + jnp.sum((z * v).reshape(16, 8, 128), axis=0)
        return rate_sum, skip_sum

    zero = jnp.zeros((8, 128), F32)
    sums = lax.fori_loop(0, GROUPS // 4, step, (zero, zero))
    lane = lax.broadcasted_iota(jnp.int32, (8, 128), 1)
    first = (my_y * NZ + my_z) * 2
    result = zero
    for kind in range(2):
        for head in range(2):
            picked = jnp.where((lane >= HEAD) if head else (lane < HEAD), sums[kind], 0.0)
            value = jnp.sum(picked, keepdims=True)
            result = jnp.where(lane == kind * H + first + head, value, result)
    out_ref[...] = result


def table_scratch(with_sums):
    square = pltpu.VMEM((GROUPS, Q, 128), F32)
    return [
        pltpu.VMEM((GROUPS, 2 * N, 128), BF16),
        pltpu.VMEM((GROUPS, Q, 256), BF16),
        pltpu.VMEM((GROUPS, N, Q), BF16),
        square,
        square,
        *([square] if with_sums else []),
        pltpu.VMEM((GROUPS, 8, 128), F32),
    ]


def series(pos, rows, pieces, rate):
    return pl.pallas_call(
        series_kernel,
        in_specs=[SMEM, full(rows.shape), HBM, HBM, HBM, HBM, HBM, full(rate.shape)],
        out_specs=full((GROUPS, Q, 128)),
        out_shape=jax.ShapeDtypeStruct((GROUPS, Q, 128), BF16),
        scratch_shapes=[
            *table_scratch(False),
            pltpu.VMEM((GROUPS, Q, 128), BF16),
            pltpu.VMEM((GROUPS, Q, 128), F32),
            pltpu.VMEM((N, 128), F32),
            pltpu.SemaphoreType.DMA,
        ],
        name="series",
        cost_estimate=pl.CostEstimate(flops=3_000_000_000, transcendentals=1_000_000, bytes_accessed=5_000_000),
    )(pos, rows, *pieces, rate)


def tangents(pos, rows, summed, pieces, rate):
    return pl.pallas_call(
        tangent_kernel,
        in_specs=[SMEM, full(rows.shape), full(summed.shape), HBM, HBM, HBM, HBM, HBM, full(rate.shape)],
        out_specs=full((GROUPS, Q, 128)),
        out_shape=jax.ShapeDtypeStruct((GROUPS, Q, 128), F32),
        scratch_shapes=[*table_scratch(True), pltpu.VMEM((N, 256), F32), pltpu.SemaphoreType.DMA],
        name="tangents",
        cost_estimate=pl.CostEstimate(flops=2_000_000_000, transcendentals=1_000_000, bytes_accessed=5_000_000),
    )(pos, rows, summed, *pieces, rate)


def dots(pos, summed, change, lines, planes):
    return pl.pallas_call(
        dots_kernel,
        in_specs=[SMEM, full(summed.shape), full(change.shape), *[HBM] * (NZ + NY - 1)],
        out_specs=full((8, 128)),
        out_shape=jax.ShapeDtypeStruct((8, 128), F32),
        scratch_shapes=[pltpu.VMEM((GROUPS, Q, 128), BF16), pltpu.SemaphoreType.DMA],
        name="dots",
        cost_estimate=pl.CostEstimate(flops=2_000_000, transcendentals=0, bytes_accessed=4_000_000),
    )(pos, summed, change, *lines, *planes)


def near(by, size):
    return by if by <= size // 2 else by - size


def gather_line(input_map, output_map):
    own = jnp.concatenate([input_map, output_map], axis=0)[None]
    last, after = shifted(own, "seq_1", 1), shifted(own, "seq_1", -1)
    far_last = shifted(jnp.concatenate([last, own]), "seq_1", 2)
    far_after = shifted(jnp.concatenate([own, after]), "seq_1", -2)
    far = shifted(own, "seq_1", 4)
    return jnp.concatenate([own, after, far_after, far, far_last, last])


def gather_plane(line):
    from_next = shifted(line, "seq_0", -1)
    from_last = shifted(line, "seq_0", 1)
    low = shifted(from_last[:4], "seq_0", 1)
    high = shifted(from_next[4:], "seq_0", -1)
    return line, from_next, from_last, low, high


def inner(cotangent, fixed_point, input_map, output_map, step_size, forget, decay_rate, skip_gain):
    my_y, my_z = lax.axis_index("seq_0"), lax.axis_index("seq_1")
    pos = jnp.stack([my_y, my_z]).astype(jnp.int32)
    first = (my_y * NZ + my_z) * 2
    own = jnp.stack([lax.dynamic_slice_in_dim(a, first, 2) for a in (decay_rate, skip_gain)])
    rate = jnp.repeat(own, HEAD, axis=1)

    line = gather_line(input_map[0], output_map[0])
    packed, line = lax.optimization_barrier((pack(cotangent[0], step_size[0], forget), line))
    pieces = gather_plane(line)
    rows = lax.all_to_all(packed, SEQ, split_axis=0, concat_axis=0, tiled=True)
    own_lines = split(pos, fixed_point[0])
    lines = [own_lines[0]] + [shifted(own_lines[d], "seq_1", near(d, NZ)) for d in range(1, NZ)]
    summed = series(pos, rows, pieces, rate)
    result = lax.all_to_all(summed, SEQ, split_axis=0, concat_axis=0, tiled=True)
    change = tangents(pos, rows, summed, pieces, rate)
    planes = []
    for d in range(1, NY):
        stacked = jnp.concatenate([x[d : d + 1] for x in lines])
        planes.append(shifted(stacked, "seq_0", near(d, NY)))
    totals = dots(pos, summed, change, lines, planes)
    for axis in BATCH:
        bit = 1
        while bit < lax.axis_size(axis):
            totals = totals + swapped(totals, axis, bit)
            bit *= 2
    copies = jnp.broadcast_to(totals[:1], (GROUPS, 1, 128))
    totals = lax.all_to_all(copies, SEQ, split_axis=0, concat_axis=0, tiled=True)
    totals = jnp.sum(totals, axis=(0, 1)) * (1.0 / (lax.axis_size(BATCH) * Q * GROUPS))
    return join(result)[None], totals[:H], totals[H:]


def solution(mesh):
    torus = Mesh(mesh.devices.reshape(4, 2, 4, 8), ("batch_0", "batch_1", "seq_0", "seq_1"))
    return jax.shard_map(
        inner,
        mesh=torus,
        in_specs=(
            P(BATCH, SEQ, None),
            P(BATCH, SEQ, None),
            P(BATCH, SEQ, None),
            P(BATCH, SEQ, None),
            P(BATCH, None, SEQ),
            P(BATCH, SEQ),
            P(),
            P(),
        ),
        out_specs=(P(BATCH, SEQ, None), P(), P()),
        check_vma=False,
    )
```

```python
import jax
import jax.numpy as jnp
from jax import lax
from jax.experimental import pallas as pl
from jax.experimental.pallas import tpu as pltpu
from jax.sharding import Mesh
from jax.sharding import PartitionSpec as P

H = 64
HEAD = 64
N = 128
Q = 128
EXTRA = 8
GROUPS = 32
NY = 4
NZ = 8
UNROLL = 16
PREP = 16
PAIRED = 8
SEQ = ("seq_0", "seq_1")
BATCH = ("batch_0", "batch_1")
F32 = jnp.float32
BF16 = jnp.bfloat16


def shifted(x, axis, by):
    size = lax.axis_size(axis)
    return lax.ppermute(x, axis, [(i, (i + by) % size) for i in range(size)])


def swapped(x, axis, bit):
    size = lax.axis_size(axis)
    return lax.ppermute(x, axis, [(i, i ^ bit) for i in range(size)])


def full(shape):
    return pl.BlockSpec(shape, lambda *_: (0,) * len(shape))


HBM = pl.BlockSpec(memory_space=pltpu.HBM)
SMEM = pl.BlockSpec(memory_space=pltpu.SMEM)


def halves(x):
    high = x.astype(BF16)
    return high, (x - high.astype(F32)).astype(BF16)


def pack_kernel(step_ref, forget_ref, cot_ref, out_ref, sem):
    copies = [
        pltpu.make_async_copy(cot_ref.at[:, pl.ds(j * 128, 128)], out_ref.at[j, pl.ds(0, Q), :], sem)
        for j in range(GROUPS)
    ]
    for c in copies:
        c.start()
    step_high, step_low = halves(step_ref[...])
    step_high, step_low = step_high.astype(F32), step_low.astype(F32)
    tail = [f.astype(F32) for f in halves(forget_ref[...])] + [jnp.zeros((2, Q), F32)]
    for j in range(GROUPS):
        two = slice(2 * j, 2 * j + 2)
        rows = jnp.concatenate([step_high[two], step_low[two], *tail], axis=0)
        out_ref[j, Q : Q + EXTRA, :] = rows.astype(BF16)
    for c in copies:
        c.wait()


def pack(cot, step, forget):
    return pl.pallas_call(
        pack_kernel,
        in_specs=[full(step.shape), full(forget.shape), HBM],
        out_specs=full((GROUPS, Q + EXTRA, 128)),
        out_shape=jax.ShapeDtypeStruct((GROUPS, Q + EXTRA, 128), BF16),
        scratch_shapes=[pltpu.SemaphoreType.DMA],
        name="pack",
    )(step, forget, cot)


def split_kernel(in_ref, out_ref, sem):
    copies = [
        pltpu.make_async_copy(in_ref.at[:, pl.ds(j * 128, 128)], out_ref.at[j], sem) for j in range(GROUPS)
    ]
    for c in copies:
        c.start()
    for c in copies:
        c.wait()


def split(x):
    return pl.pallas_call(
        split_kernel,
        in_specs=[HBM],
        out_specs=full((GROUPS, Q, 128)),
        out_shape=jax.ShapeDtypeStruct((GROUPS, Q, 128), BF16),
        scratch_shapes=[pltpu.SemaphoreType.DMA],
        name="split",
    )(x)


def join_kernel(in_ref, out_ref, sem):
    copies = [
        pltpu.make_async_copy(in_ref.at[j], out_ref.at[:, pl.ds(j * 128, 128)], sem) for j in range(GROUPS)
    ]
    for c in copies:
        c.start()
    for c in copies:
        c.wait()


def join(x):
    return pl.pallas_call(
        join_kernel,
        in_specs=[full(x.shape)],
        out_specs=HBM,
        out_shape=jax.ShapeDtypeStruct((Q, GROUPS * 128), BF16),
        scratch_shapes=[pltpu.SemaphoreType.DMA],
        name="join",
    )(x)


def dot(a, b):
    return lax.dot_general(a, b, (((1,), (0,)), ((), ())), preferred_element_type=F32)


def dot_t(a, b):
    return lax.dot_general(a, b, (((1,), (1,)), ((), ())), preferred_element_type=F32)


def fetch_maps(pos_ref, pieces, maps_ref, sem):
    my_y, my_z = pos_ref[0], pos_ref[1]
    copies = []
    for dy in range(NY):
        for dz in range(NZ):
            if dy == 0:
                source = pieces[0].at[dz]
            elif dy == 1:
                source = pieces[1].at[dz]
            elif dy == 3:
                source = pieces[2].at[dz]
            else:
                source = pieces[3].at[dz] if dz < 4 else pieces[4].at[dz - 4]
            place = ((my_y + dy) % NY) * NZ + (my_z + dz) % NZ
            copies.append(pltpu.make_async_copy(source, maps_ref.at[place], sem))
    for c in copies:
        c.start()
    for c in copies:
        c.wait()


def constants():
    rows = lax.broadcasted_iota(jnp.int32, (Q, Q), 0)
    cols = lax.broadcasted_iota(jnp.int32, (Q, Q), 1)
    lower = (rows >= cols).astype(F32).astype(BF16)
    same = (rows == cols).astype(F32).astype(BF16)
    return rows <= cols, lower, same


def prepare(c, in_ref, maps_ref, rate_ref, consts, mat_ref, turn_ref, e_ref, g_ref, s_ref, m_ref):
    upper, lower, same = consts
    both = maps_ref[c]
    b_rows, c_rows = both[:N], both[N:]
    prod = dot_t(jnp.concatenate([b_rows, same], axis=0), c_rows)
    mat_ref[c, :, :N] = jnp.where(upper, prod[:Q], 0.0).astype(BF16)
    mat_ref[c, :, N:] = b_rows
    turn_ref[c] = prod[Q:].astype(BF16)
    rows = in_ref[c, Q : Q + EXTRA, :].astype(F32)

    def wide(first, second):
        return jnp.concatenate(
            [jnp.broadcast_to(rows[first : first + 1], (HEAD, Q)), jnp.broadcast_to(rows[second : second + 1], (HEAD, Q))],
            axis=0,
        ).astype(BF16)

    steps = jnp.concatenate([wide(0, 1), wide(2, 3)], axis=1)
    forgets = jnp.concatenate([wide(4, 4), wide(5, 5)], axis=1)
    lower_twice = jnp.concatenate([lower, lower], axis=1)
    same_twice = jnp.concatenate([same, same], axis=1)
    sums = dot_t(jnp.concatenate([lower_twice, same_twice], axis=0), steps)
    step_sum, step_col = sums[:Q], sums[Q:]
    forget_sum = dot_t(lower_twice, forgets)
    log_decay = -(rate_ref[0:1, :] * step_sum + forget_sum)
    middle = 0.5 * log_decay[Q - 1 : Q, :]
    gap = log_decay - middle
    e_ref[c] = jnp.exp(gap)
    g_ref[c] = step_col * jnp.exp(-gap)
    if s_ref is not None:
        s_ref[c] = step_sum
    m_ref[c] = jnp.broadcast_to(jnp.exp(middle), (8, 128))


def series_kernel(pos_ref, in_ref, p0, p1, p2, p3, p4, rate_ref, out_ref, maps_ref, mat_ref, turn_ref, e_ref, g_ref, m_ref, v_ref, sum_ref, back_ref, sem):
    fetch_maps(pos_ref, (p0, p1, p2, p3, p4), maps_ref, sem)
    consts = constants()

    def prep(i, _):
        for j in range(PREP):
            prepare(i * PREP + j, in_ref, maps_ref, rate_ref, consts, mat_ref, turn_ref, e_ref, g_ref, None, m_ref)
        return 0

    lax.fori_loop(0, GROUPS // PREP, prep, 0)
    skip = rate_ref[1:2, :]
    for k in range(3):
        back_ref[...] = jnp.zeros((N, 128), F32)

        def step(i, _):
            groups = [GROUPS - 1 - (i * UNROLL + j) for j in range(UNROLL)]
            values = [(in_ref[c, :Q, :] if k == 0 else v_ref[c]).astype(F32) for c in groups]
            turned = [(e_ref[c] * v).astype(BF16) for c, v in zip(groups, values)]
            local = [dot(turn_ref[c], x) for c, x in zip(groups, turned)]
            back = back_ref[...]
            states = []
            for j, c in enumerate(groups):
                states.append(back.astype(BF16))
                scale = m_ref[c, 0:1, :] * m_ref[jnp.maximum(c - 1, 0), 0:1, :]
                back = scale * (back + local[j])
            back_ref[...] = back
            mixed = [
                dot(mat_ref[c], jnp.concatenate([x, b], axis=0)) for c, x, b in zip(groups, turned, states)
            ]
            fresh = [
                (g_ref[c] * r + skip * v).astype(BF16) for c, r, v in zip(groups, mixed, values)
            ]
            totals = [
                (v if k == 0 else sum_ref[c]) + n.astype(F32) for c, v, n in zip(groups, values, fresh)
            ]
            for c, n, t in zip(groups, fresh, totals):
                if k < 2:
                    v_ref[c] = n
                    sum_ref[c] = t
                else:
                    out_ref[c] = t.astype(BF16)
            return 0

        lax.fori_loop(0, GROUPS // UNROLL, step, 0)


def rate_kernel(pos_ref, in_ref, sum_ref, fixed_ref, p0, p1, p2, p3, p4, rate_ref, out_ref, maps_ref, mat_ref, turn_ref, e_ref, g_ref, s_ref, m_ref, back_ref, acc_ref, sem):
    fetch_maps(pos_ref, (p0, p1, p2, p3, p4), maps_ref, sem)
    consts = constants()

    def prep(i, _):
        for j in range(PREP):
            prepare(i * PREP + j, in_ref, maps_ref, rate_ref, consts, mat_ref, turn_ref, e_ref, g_ref, s_ref, m_ref)
        return 0

    lax.fori_loop(0, GROUPS // PREP, prep, 0)
    back_ref[...] = jnp.zeros((N, 256), F32)
    acc_ref[...] = jnp.zeros((2, 8, 128), F32)

    def step(i, _):
        groups = [GROUPS - 1 - (i * PAIRED + j) for j in range(PAIRED)]
        values = [sum_ref[c].astype(F32) for c in groups]
        turned = []
        for c, v in zip(groups, values):
            ev = e_ref[c] * v
            turned.append(jnp.concatenate([ev.astype(BF16), (ev * s_ref[c]).astype(BF16)], axis=1))
        local = [dot(turn_ref[c], x) for c, x in zip(groups, turned)]
        back, tangent = back_ref[:, :128], back_ref[:, 128:]
        states = []
        for j, c in enumerate(groups):
            tangent = tangent + s_ref[c, Q - 1 : Q, :] * back
            states.append(jnp.concatenate([back.astype(BF16), tangent.astype(BF16)], axis=1))
            scale = m_ref[c, 0:1, :] * m_ref[jnp.maximum(c - 1, 0), 0:1, :]
            back = scale * (back + local[j][:, :128])
            tangent = scale * (tangent + local[j][:, 128:])
        back_ref[:, :128] = back
        back_ref[:, 128:] = tangent
        mixed = [dot(mat_ref[c], jnp.concatenate([x, b], axis=0)) for c, x, b in zip(groups, turned, states)]
        rate_sum, skip_sum = acc_ref[0], acc_ref[1]
        for c, v, r in zip(groups, values, mixed):
            z = fixed_ref[c].astype(F32)
            change = g_ref[c] * (r[:, 128:] - s_ref[c] * r[:, :128])
            rate_sum = rate_sum + jnp.sum((z * change).reshape(16, 8, 128), axis=0)
            skip_sum = skip_sum + jnp.sum((z * v).reshape(16, 8, 128), axis=0)
        acc_ref[0] = rate_sum
        acc_ref[1] = skip_sum
        return 0

    lax.fori_loop(0, GROUPS // PAIRED, step, 0)
    lane = lax.broadcasted_iota(jnp.int32, (8, 128), 1)
    first = (pos_ref[0] * NZ + pos_ref[1]) * 2
    result = jnp.zeros((8, 128), F32)
    for kind in range(2):
        for head in range(2):
            picked = jnp.where((lane >= HEAD) if head else (lane < HEAD), acc_ref[kind], 0.0)
            value = jnp.sum(picked, keepdims=True)
            value = -value if kind == 0 else value
            result = jnp.where(lane == kind * H + first + head, value, result)
    out_ref[...] = result


def table_scratch(with_sums):
    square = pltpu.VMEM((GROUPS, Q, 128), F32)
    return [
        pltpu.VMEM((GROUPS, 2 * N, 128), BF16),
        pltpu.VMEM((GROUPS, Q, 256), BF16),
        pltpu.VMEM((GROUPS, N, Q), BF16),
        square,
        square,
        *([square] if with_sums else []),
        pltpu.VMEM((GROUPS, 8, 128), F32),
    ]


def series(pos, rows, pieces, rate):
    return pl.pallas_call(
        series_kernel,
        in_specs=[SMEM, full(rows.shape), HBM, HBM, HBM, HBM, HBM, full(rate.shape)],
        out_specs=full((GROUPS, Q, 128)),
        out_shape=jax.ShapeDtypeStruct((GROUPS, Q, 128), BF16),
        scratch_shapes=[
            *table_scratch(False),
            pltpu.VMEM((GROUPS, Q, 128), BF16),
            pltpu.VMEM((GROUPS, Q, 128), F32),
            pltpu.VMEM((N, 128), F32),
            pltpu.SemaphoreType.DMA,
        ],
        name="series",
        cost_estimate=pl.CostEstimate(flops=3_000_000_000, transcendentals=1_000_000, bytes_accessed=5_000_000),
    )(pos, rows, *pieces, rate)


def rates(pos, rows, summed, fixed, pieces, rate):
    return pl.pallas_call(
        rate_kernel,
        in_specs=[SMEM, full(rows.shape), full(summed.shape), full(fixed.shape), HBM, HBM, HBM, HBM, HBM, full(rate.shape)],
        out_specs=full((8, 128)),
        out_shape=jax.ShapeDtypeStruct((8, 128), F32),
        scratch_shapes=[
            *table_scratch(True),
            pltpu.VMEM((N, 256), F32),
            pltpu.VMEM((2, 8, 128), F32),
            pltpu.SemaphoreType.DMA,
        ],
        name="rates",
        cost_estimate=pl.CostEstimate(flops=2_000_000_000, transcendentals=1_000_000, bytes_accessed=5_000_000),
    )(pos, rows, summed, fixed, *pieces, rate)


def gather_line(input_map, output_map):
    own = jnp.concatenate([input_map, output_map], axis=0)[None]
    last, after = shifted(own, "seq_1", 1), shifted(own, "seq_1", -1)
    far_last = shifted(jnp.concatenate([last, own]), "seq_1", 2)
    far_after = shifted(jnp.concatenate([own, after]), "seq_1", -2)
    far = shifted(own, "seq_1", 4)
    return jnp.concatenate([own, after, far_after, far, far_last, last])


def gather_plane(line):
    from_next = shifted(line, "seq_0", -1)
    from_last = shifted(line, "seq_0", 1)
    low = shifted(from_last[:4], "seq_0", 1)
    high = shifted(from_next[4:], "seq_0", -1)
    return line, from_next, from_last, low, high


def inner(cotangent, fixed_point, input_map, output_map, step_size, forget, decay_rate, skip_gain):
    my_y, my_z = lax.axis_index("seq_0"), lax.axis_index("seq_1")
    pos = jnp.stack([my_y, my_z]).astype(jnp.int32)
    first = (my_y * NZ + my_z) * 2
    own = jnp.stack([lax.dynamic_slice_in_dim(a, first, 2) for a in (decay_rate, skip_gain)])
    rate = jnp.repeat(own, HEAD, axis=1)

    line = gather_line(input_map[0], output_map[0])
    packed = pack(cotangent[0], step_size[0], forget)
    pieces = gather_plane(line)
    rows = lax.all_to_all(packed, SEQ, split_axis=0, concat_axis=0, tiled=True)
    fixed = lax.all_to_all(split(fixed_point[0]), SEQ, split_axis=0, concat_axis=0, tiled=True)
    summed = series(pos, rows, pieces, rate)
    result = lax.all_to_all(summed, SEQ, split_axis=0, concat_axis=0, tiled=True)
    totals = rates(pos, rows, summed, fixed, pieces, rate)
    for axis in BATCH:
        bit = 1
        while bit < lax.axis_size(axis):
            totals = totals + swapped(totals, axis, bit)
            bit *= 2
    copies = jnp.broadcast_to(totals[:1], (GROUPS, 1, 128))
    totals = lax.all_to_all(copies, SEQ, split_axis=0, concat_axis=0, tiled=True)
    totals = jnp.sum(totals, axis=(0, 1)) * (1.0 / (lax.axis_size(BATCH) * Q * GROUPS))
    return join(result)[None], totals[:H], totals[H:]


def solution(mesh):
    torus = Mesh(mesh.devices.reshape(4, 2, 4, 8), ("batch_0", "batch_1", "seq_0", "seq_1"))
    return jax.shard_map(
        inner,
        mesh=torus,
        in_specs=(
            P(BATCH, SEQ, None),
            P(BATCH, SEQ, None),
            P(BATCH, SEQ, None),
            P(BATCH, SEQ, None),
            P(BATCH, None, SEQ),
            P(BATCH, SEQ),
            P(),
            P(),
        ),
        out_specs=(P(BATCH, SEQ, None), P(), P()),
        check_vma=False,
    )
```

```python
import jax
import jax.numpy as jnp
from jax import lax
from jax.experimental import pallas as pl
from jax.experimental.pallas import tpu as pltpu
from jax.sharding import Mesh
from jax.sharding import PartitionSpec as P

H = 64
HEAD = 64
N = 128
Q = 128
EXTRA = 8
GROUPS = 32
NZ = 8
UNROLL = 16
PREP = 16
PAIRED = 8
SEQ = ("seq_0", "seq_1")
BATCH = ("batch_0", "batch_1")
F32 = jnp.float32
BF16 = jnp.bfloat16


def swapped(x, axis, bit):
    size = lax.axis_size(axis)
    return lax.ppermute(x, axis, [(i, i ^ bit) for i in range(size)])


def full(shape):
    return pl.BlockSpec(shape, lambda *_: (0,) * len(shape))


HBM = pl.BlockSpec(memory_space=pltpu.HBM)
SMEM = pl.BlockSpec(memory_space=pltpu.SMEM)


def halves(x):
    high = x.astype(BF16)
    return high, (x - high.astype(F32)).astype(BF16)


def pack_kernel(step_ref, forget_ref, cot_ref, out_ref, sem):
    copies = [
        pltpu.make_async_copy(cot_ref.at[:, pl.ds(j * 128, 128)], out_ref.at[j, pl.ds(0, Q), :], sem)
        for j in range(GROUPS)
    ]
    for c in copies:
        c.start()
    step_high, step_low = halves(step_ref[...])
    step_high, step_low = step_high.astype(F32), step_low.astype(F32)
    tail = [f.astype(F32) for f in halves(forget_ref[...])] + [jnp.zeros((2, Q), F32)]
    for j in range(GROUPS):
        two = slice(2 * j, 2 * j + 2)
        rows = jnp.concatenate([step_high[two], step_low[two], *tail], axis=0)
        out_ref[j, Q : Q + EXTRA, :] = rows.astype(BF16)
    for c in copies:
        c.wait()


def pack(cot, step, forget):
    return pl.pallas_call(
        pack_kernel,
        in_specs=[full(step.shape), full(forget.shape), HBM],
        out_specs=full((GROUPS, Q + EXTRA, 128)),
        out_shape=jax.ShapeDtypeStruct((GROUPS, Q + EXTRA, 128), BF16),
        scratch_shapes=[pltpu.SemaphoreType.DMA],
        name="pack",
    )(step, forget, cot)


def split_kernel(in_ref, out_ref, sem):
    copies = [
        pltpu.make_async_copy(in_ref.at[:, pl.ds(j * 128, 128)], out_ref.at[j], sem) for j in range(GROUPS)
    ]
    for c in copies:
        c.start()
    for c in copies:
        c.wait()


def split(x):
    return pl.pallas_call(
        split_kernel,
        in_specs=[HBM],
        out_specs=full((GROUPS, Q, 128)),
        out_shape=jax.ShapeDtypeStruct((GROUPS, Q, 128), BF16),
        scratch_shapes=[pltpu.SemaphoreType.DMA],
        name="split",
    )(x)


def join_kernel(in_ref, out_ref, sem):
    copies = [
        pltpu.make_async_copy(in_ref.at[j], out_ref.at[:, pl.ds(j * 128, 128)], sem) for j in range(GROUPS)
    ]
    for c in copies:
        c.start()
    for c in copies:
        c.wait()


def join(x):
    return pl.pallas_call(
        join_kernel,
        in_specs=[full(x.shape)],
        out_specs=HBM,
        out_shape=jax.ShapeDtypeStruct((Q, GROUPS * 128), BF16),
        scratch_shapes=[pltpu.SemaphoreType.DMA],
        name="join",
    )(x)


def dot(a, b):
    return lax.dot_general(a, b, (((1,), (0,)), ((), ())), preferred_element_type=F32)


def dot_t(a, b):
    return lax.dot_general(a, b, (((1,), (1,)), ((), ())), preferred_element_type=F32)


def constants():
    rows = lax.broadcasted_iota(jnp.int32, (Q, Q), 0)
    cols = lax.broadcasted_iota(jnp.int32, (Q, Q), 1)
    lower = (rows >= cols).astype(F32).astype(BF16)
    same = (rows == cols).astype(F32).astype(BF16)
    return rows <= cols, lower, same


def prepare(c, in_ref, maps_ref, rate_ref, consts, mat_ref, turn_ref, e_ref, g_ref, s_ref, m_ref):
    upper, lower, same = consts
    both = maps_ref[c]
    b_rows, c_rows = both[:N], both[N:]
    prod = dot_t(jnp.concatenate([b_rows, same], axis=0), c_rows)
    mat_ref[c, :, :N] = jnp.where(upper, prod[:Q], 0.0).astype(BF16)
    mat_ref[c, :, N:] = b_rows
    turn_ref[c] = prod[Q:].astype(BF16)
    rows = in_ref[c, Q : Q + EXTRA, :].astype(F32)

    def wide(first, second):
        return jnp.concatenate(
            [jnp.broadcast_to(rows[first : first + 1], (HEAD, Q)), jnp.broadcast_to(rows[second : second + 1], (HEAD, Q))],
            axis=0,
        ).astype(BF16)

    steps = jnp.concatenate([wide(0, 1), wide(2, 3)], axis=1)
    forgets = jnp.concatenate([wide(4, 4), wide(5, 5)], axis=1)
    lower_twice = jnp.concatenate([lower, lower], axis=1)
    same_twice = jnp.concatenate([same, same], axis=1)
    sums = dot_t(jnp.concatenate([lower_twice, same_twice], axis=0), steps)
    step_sum, step_col = sums[:Q], sums[Q:]
    forget_sum = dot_t(lower_twice, forgets)
    log_decay = -(rate_ref[0:1, :] * step_sum + forget_sum)
    middle = 0.5 * log_decay[Q - 1 : Q, :]
    gap = log_decay - middle
    e_ref[c] = jnp.exp(gap)
    g_ref[c] = step_col * jnp.exp(-gap)
    if s_ref is not None:
        s_ref[c] = step_sum
    m_ref[c] = jnp.broadcast_to(jnp.exp(middle), (8, 128))


def series_kernel(in_ref, maps_ref, rate_ref, out_ref, mat_ref, turn_ref, e_ref, g_ref, m_ref, v_ref, sum_ref, back_ref):
    consts = constants()

    def prep(i, _):
        for j in range(PREP):
            prepare(i * PREP + j, in_ref, maps_ref, rate_ref, consts, mat_ref, turn_ref, e_ref, g_ref, None, m_ref)
        return 0

    lax.fori_loop(0, GROUPS // PREP, prep, 0)
    skip = rate_ref[1:2, :]
    for k in range(3):
        back_ref[...] = jnp.zeros((N, 128), F32)

        def step(i, _):
            groups = [GROUPS - 1 - (i * UNROLL + j) for j in range(UNROLL)]
            values = [(in_ref[c, :Q, :] if k == 0 else v_ref[c]).astype(F32) for c in groups]
            turned = [(e_ref[c] * v).astype(BF16) for c, v in zip(groups, values)]
            local = [dot(turn_ref[c], x) for c, x in zip(groups, turned)]
            back = back_ref[...]
            states = []
            for j, c in enumerate(groups):
                states.append(back.astype(BF16))
                scale = m_ref[c, 0:1, :] * m_ref[jnp.maximum(c - 1, 0), 0:1, :]
                back = scale * (back + local[j])
            back_ref[...] = back
            mixed = [
                dot(mat_ref[c], jnp.concatenate([x, b], axis=0)) for c, x, b in zip(groups, turned, states)
            ]
            fresh = [
                (g_ref[c] * r + skip * v).astype(BF16) for c, r, v in zip(groups, mixed, values)
            ]
            totals = [
                (v if k == 0 else sum_ref[c]) + n.astype(F32) for c, v, n in zip(groups, values, fresh)
            ]
            for c, n, t in zip(groups, fresh, totals):
                if k < 2:
                    v_ref[c] = n
                    sum_ref[c] = t
                else:
                    out_ref[c] = t.astype(BF16)
            return 0

        lax.fori_loop(0, GROUPS // UNROLL, step, 0)


def rate_kernel(pos_ref, in_ref, sum_ref, fixed_ref, maps_ref, rate_ref, out_ref, mat_ref, turn_ref, e_ref, g_ref, s_ref, m_ref, back_ref, acc_ref):
    consts = constants()

    def prep(i, _):
        for j in range(PREP):
            prepare(i * PREP + j, in_ref, maps_ref, rate_ref, consts, mat_ref, turn_ref, e_ref, g_ref, s_ref, m_ref)
        return 0

    lax.fori_loop(0, GROUPS // PREP, prep, 0)
    back_ref[...] = jnp.zeros((N, 256), F32)
    acc_ref[...] = jnp.zeros((2, 8, 128), F32)

    def step(i, _):
        groups = [GROUPS - 1 - (i * PAIRED + j) for j in range(PAIRED)]
        values = [sum_ref[c].astype(F32) for c in groups]
        turned = []
        for c, v in zip(groups, values):
            ev = e_ref[c] * v
            turned.append(jnp.concatenate([ev.astype(BF16), (ev * s_ref[c]).astype(BF16)], axis=1))
        local = [dot(turn_ref[c], x) for c, x in zip(groups, turned)]
        back, tangent = back_ref[:, :128], back_ref[:, 128:]
        states = []
        for j, c in enumerate(groups):
            tangent = tangent + s_ref[c, Q - 1 : Q, :] * back
            states.append(jnp.concatenate([back.astype(BF16), tangent.astype(BF16)], axis=1))
            scale = m_ref[c, 0:1, :] * m_ref[jnp.maximum(c - 1, 0), 0:1, :]
            back = scale * (back + local[j][:, :128])
            tangent = scale * (tangent + local[j][:, 128:])
        back_ref[:, :128] = back
        back_ref[:, 128:] = tangent
        mixed = [dot(mat_ref[c], jnp.concatenate([x, b], axis=0)) for c, x, b in zip(groups, turned, states)]
        rate_sum, skip_sum = acc_ref[0], acc_ref[1]
        for c, v, r in zip(groups, values, mixed):
            z = fixed_ref[c].astype(F32)
            change = g_ref[c] * (r[:, 128:] - s_ref[c] * r[:, :128])
            rate_sum = rate_sum + jnp.sum((z * change).reshape(16, 8, 128), axis=0)
            skip_sum = skip_sum + jnp.sum((z * v).reshape(16, 8, 128), axis=0)
        acc_ref[0] = rate_sum
        acc_ref[1] = skip_sum
        return 0

    lax.fori_loop(0, GROUPS // PAIRED, step, 0)
    lane = lax.broadcasted_iota(jnp.int32, (8, 128), 1)
    first = (pos_ref[0] * NZ + pos_ref[1]) * 2
    result = jnp.zeros((8, 128), F32)
    for kind in range(2):
        for head in range(2):
            picked = jnp.where((lane >= HEAD) if head else (lane < HEAD), acc_ref[kind], 0.0)
            value = jnp.sum(picked, keepdims=True)
            value = -value if kind == 0 else value
            result = jnp.where(lane == kind * H + first + head, value, result)
    out_ref[...] = result


def table_scratch(with_sums):
    square = pltpu.VMEM((GROUPS, Q, 128), F32)
    return [
        pltpu.VMEM((GROUPS, Q, 256), BF16),
        pltpu.VMEM((GROUPS, N, Q), BF16),
        square,
        square,
        *([square] if with_sums else []),
        pltpu.VMEM((GROUPS, 8, 128), F32),
    ]


def series(rows, maps, rate):
    return pl.pallas_call(
        series_kernel,
        in_specs=[full(rows.shape), full(maps.shape), full(rate.shape)],
        out_specs=full((GROUPS, Q, 128)),
        out_shape=jax.ShapeDtypeStruct((GROUPS, Q, 128), BF16),
        scratch_shapes=[
            *table_scratch(False),
            pltpu.VMEM((GROUPS, Q, 128), BF16),
            pltpu.VMEM((GROUPS, Q, 128), F32),
            pltpu.VMEM((N, 128), F32),
        ],
        name="series",
        cost_estimate=pl.CostEstimate(flops=3_000_000_000, transcendentals=1_000_000, bytes_accessed=5_000_000),
    )(rows, maps, rate)


def rates(pos, rows, summed, fixed, maps, rate):
    return pl.pallas_call(
        rate_kernel,
        in_specs=[SMEM, full(rows.shape), full(summed.shape), full(fixed.shape), full(maps.shape), full(rate.shape)],
        out_specs=full((8, 128)),
        out_shape=jax.ShapeDtypeStruct((8, 128), F32),
        scratch_shapes=[*table_scratch(True), pltpu.VMEM((N, 256), F32), pltpu.VMEM((2, 8, 128), F32)],
        name="rates",
        cost_estimate=pl.CostEstimate(flops=2_000_000_000, transcendentals=1_000_000, bytes_accessed=5_000_000),
    )(pos, rows, summed, fixed, maps, rate)


def inner(cotangent, fixed_point, input_map, output_map, step_size, forget, decay_rate, skip_gain):
    my_y, my_z = lax.axis_index("seq_0"), lax.axis_index("seq_1")
    pos = jnp.stack([my_y, my_z]).astype(jnp.int32)
    first = (my_y * NZ + my_z) * 2
    own = jnp.stack([lax.dynamic_slice_in_dim(a, first, 2) for a in (decay_rate, skip_gain)])
    rate = jnp.repeat(own, HEAD, axis=1)

    both_maps = jnp.concatenate([input_map[0], output_map[0]], axis=0)
    maps = lax.all_gather(both_maps, SEQ, axis=0, tiled=True).reshape(GROUPS, 2 * N, 128)
    packed = pack(cotangent[0], step_size[0], forget)
    rows = lax.all_to_all(packed, SEQ, split_axis=0, concat_axis=0, tiled=True)
    fixed = lax.all_to_all(split(fixed_point[0]), SEQ, split_axis=0, concat_axis=0, tiled=True)
    summed = series(rows, maps, rate)
    result = lax.all_to_all(summed, SEQ, split_axis=0, concat_axis=0, tiled=True)
    totals = rates(pos, rows, summed, fixed, maps, rate)
    for axis in BATCH:
        bit = 1
        while bit < lax.axis_size(axis):
            totals = totals + swapped(totals, axis, bit)
            bit *= 2
    copies = jnp.broadcast_to(totals[:1], (GROUPS, 1, 128))
    totals = lax.all_to_all(copies, SEQ, split_axis=0, concat_axis=0, tiled=True)
    totals = jnp.sum(totals, axis=(0, 1)) * (1.0 / (lax.axis_size(BATCH) * Q * GROUPS))
    return join(result)[None], totals[:H], totals[H:]


def solution(mesh):
    torus = Mesh(mesh.devices.reshape(4, 2, 4, 8), ("batch_0", "batch_1", "seq_0", "seq_1"))
    return jax.shard_map(
        inner,
        mesh=torus,
        in_specs=(
            P(BATCH, SEQ, None),
            P(BATCH, SEQ, None),
            P(BATCH, SEQ, None),
            P(BATCH, SEQ, None),
            P(BATCH, None, SEQ),
            P(BATCH, SEQ),
            P(),
            P(),
        ),
        out_specs=(P(BATCH, SEQ, None), P(), P()),
        check_vma=False,
    )
```

```python
import jax
import jax.numpy as jnp
from jax import lax
from jax.experimental import pallas as pl
from jax.experimental.pallas import tpu as pltpu
from jax.sharding import Mesh
from jax.sharding import PartitionSpec as P

H = 64
HEAD = 64
N = 128
Q = 128
EXTRA = 8
GROUPS = 32
NY = 4
NZ = 8
UNROLL = 16
PREP = 16
PAIRED = 8
SEQ = ("seq_0", "seq_1")
BATCH = ("batch_0", "batch_1")
F32 = jnp.float32
BF16 = jnp.bfloat16


def shifted(x, axis, by):
    size = lax.axis_size(axis)
    return lax.ppermute(x, axis, [(i, (i + by) % size) for i in range(size)])


def swapped(x, axis, bit):
    size = lax.axis_size(axis)
    return lax.ppermute(x, axis, [(i, i ^ bit) for i in range(size)])


def full(shape):
    return pl.BlockSpec(shape, lambda *_: (0,) * len(shape))


HBM = pl.BlockSpec(memory_space=pltpu.HBM)
SMEM = pl.BlockSpec(memory_space=pltpu.SMEM)


def halves(x):
    high = x.astype(BF16)
    return high, (x - high.astype(F32)).astype(BF16)


def pack_kernel(step_ref, forget_ref, cot_ref, fixed_ref, out_ref, sem):
    copies = []
    for j in range(GROUPS):
        lanes = pl.ds(j * 128, 128)
        copies.append(pltpu.make_async_copy(cot_ref.at[:, lanes], out_ref.at[j, pl.ds(0, Q), :], sem))
        copies.append(pltpu.make_async_copy(fixed_ref.at[:, lanes], out_ref.at[j, pl.ds(Q + EXTRA, Q), :], sem))
    for c in copies:
        c.start()
    step_high, step_low = halves(step_ref[...])
    step_high, step_low = step_high.astype(F32), step_low.astype(F32)
    tail = [f.astype(F32) for f in halves(forget_ref[...])] + [jnp.zeros((2, Q), F32)]
    for j in range(GROUPS):
        two = slice(2 * j, 2 * j + 2)
        rows = jnp.concatenate([step_high[two], step_low[two], *tail], axis=0)
        out_ref[j, Q : Q + EXTRA, :] = rows.astype(BF16)
    for c in copies:
        c.wait()


def pack(cot, fixed, step, forget):
    shape = (GROUPS, 2 * Q + EXTRA, 128)
    return pl.pallas_call(
        pack_kernel,
        in_specs=[full(step.shape), full(forget.shape), HBM, HBM],
        out_specs=full(shape),
        out_shape=jax.ShapeDtypeStruct(shape, BF16),
        scratch_shapes=[pltpu.SemaphoreType.DMA],
        name="pack",
    )(step, forget, cot, fixed)


def join_kernel(in_ref, out_ref, sem):
    copies = [
        pltpu.make_async_copy(in_ref.at[j], out_ref.at[:, pl.ds(j * 128, 128)], sem) for j in range(GROUPS)
    ]
    for c in copies:
        c.start()
    for c in copies:
        c.wait()


def join(x):
    return pl.pallas_call(
        join_kernel,
        in_specs=[full(x.shape)],
        out_specs=HBM,
        out_shape=jax.ShapeDtypeStruct((Q, GROUPS * 128), BF16),
        scratch_shapes=[pltpu.SemaphoreType.DMA],
        name="join",
    )(x)


def dot(a, b):
    return lax.dot_general(a, b, (((1,), (0,)), ((), ())), preferred_element_type=F32)


def dot_t(a, b):
    return lax.dot_general(a, b, (((1,), (1,)), ((), ())), preferred_element_type=F32)


def fetch_maps(pos_ref, pieces, maps_ref, sem):
    my_y, my_z = pos_ref[0], pos_ref[1]
    copies = []
    for dy in range(NY):
        for dz in range(NZ):
            if dy == 0:
                source = pieces[0].at[dz]
            elif dy == 1:
                source = pieces[1].at[dz]
            elif dy == 3:
                source = pieces[2].at[dz]
            else:
                source = pieces[3].at[dz] if dz < 4 else pieces[4].at[dz - 4]
            place = ((my_y + dy) % NY) * NZ + (my_z + dz) % NZ
            copies.append(pltpu.make_async_copy(source, maps_ref.at[place], sem))
    for c in copies:
        c.start()
    for c in copies:
        c.wait()


def constants():
    rows = lax.broadcasted_iota(jnp.int32, (Q, Q), 0)
    cols = lax.broadcasted_iota(jnp.int32, (Q, Q), 1)
    lower = (rows >= cols).astype(F32).astype(BF16)
    same = (rows == cols).astype(F32).astype(BF16)
    return rows <= cols, lower, same


def prepare(c, in_ref, maps_ref, rate_ref, consts, mat_ref, turn_ref, e_ref, g_ref, s_ref, m_ref):
    upper, lower, same = consts
    both = maps_ref[c]
    b_rows, c_rows = both[:N], both[N:]
    prod = dot_t(jnp.concatenate([b_rows, same], axis=0), c_rows)
    mat_ref[c, :, :N] = jnp.where(upper, prod[:Q], 0.0).astype(BF16)
    mat_ref[c, :, N:] = b_rows
    turn_ref[c] = prod[Q:].astype(BF16)
    rows = in_ref[c, Q : Q + EXTRA, :].astype(F32)

    def wide(first, second):
        return jnp.concatenate(
            [jnp.broadcast_to(rows[first : first + 1], (HEAD, Q)), jnp.broadcast_to(rows[second : second + 1], (HEAD, Q))],
            axis=0,
        ).astype(BF16)

    steps = jnp.concatenate([wide(0, 1), wide(2, 3)], axis=1)
    forgets = jnp.concatenate([wide(4, 4), wide(5, 5)], axis=1)
    lower_twice = jnp.concatenate([lower, lower], axis=1)
    same_twice = jnp.concatenate([same, same], axis=1)
    sums = dot_t(jnp.concatenate([lower_twice, same_twice], axis=0), steps)
    step_sum, step_col = sums[:Q], sums[Q:]
    forget_sum = dot_t(lower_twice, forgets)
    log_decay = -(rate_ref[0:1, :] * step_sum + forget_sum)
    middle = 0.5 * log_decay[Q - 1 : Q, :]
    gap = log_decay - middle
    e_ref[c] = jnp.exp(gap)
    g_ref[c] = step_col * jnp.exp(-gap)
    if s_ref is not None:
        s_ref[c] = step_sum
    m_ref[c] = jnp.broadcast_to(jnp.exp(middle), (8, 128))


def series_kernel(pos_ref, in_ref, p0, p1, p2, p3, p4, rate_ref, out_ref, maps_ref, mat_ref, turn_ref, e_ref, g_ref, m_ref, v_ref, sum_ref, back_ref, sem):
    fetch_maps(pos_ref, (p0, p1, p2, p3, p4), maps_ref, sem)
    consts = constants()

    def prep(i, _):
        for j in range(PREP):
            prepare(i * PREP + j, in_ref, maps_ref, rate_ref, consts, mat_ref, turn_ref, e_ref, g_ref, None, m_ref)
        return 0

    lax.fori_loop(0, GROUPS // PREP, prep, 0)
    skip = rate_ref[1:2, :]
    for k in range(3):
        back_ref[...] = jnp.zeros((N, 128), F32)

        def step(i, _):
            groups = [GROUPS - 1 - (i * UNROLL + j) for j in range(UNROLL)]
            values = [(in_ref[c, :Q, :] if k == 0 else v_ref[c]).astype(F32) for c in groups]
            turned = [(e_ref[c] * v).astype(BF16) for c, v in zip(groups, values)]
            local = [dot(turn_ref[c], x) for c, x in zip(groups, turned)]
            back = back_ref[...]
            states = []
            for j, c in enumerate(groups):
                states.append(back.astype(BF16))
                scale = m_ref[c, 0:1, :] * m_ref[jnp.maximum(c - 1, 0), 0:1, :]
                back = scale * (back + local[j])
            back_ref[...] = back
            mixed = [
                dot(mat_ref[c], jnp.concatenate([x, b], axis=0)) for c, x, b in zip(groups, turned, states)
            ]
            fresh = [
                (g_ref[c] * r + skip * v).astype(BF16) for c, r, v in zip(groups, mixed, values)
            ]
            totals = [
                (v if k == 0 else sum_ref[c]) + n.astype(F32) for c, v, n in zip(groups, values, fresh)
            ]
            for c, n, t in zip(groups, fresh, totals):
                if k < 2:
                    v_ref[c] = n
                    sum_ref[c] = t
                else:
                    out_ref[c] = t.astype(BF16)
            return 0

        lax.fori_loop(0, GROUPS // UNROLL, step, 0)


def rate_kernel(pos_ref, in_ref, sum_ref, p0, p1, p2, p3, p4, rate_ref, out_ref, maps_ref, mat_ref, turn_ref, e_ref, g_ref, s_ref, m_ref, back_ref, acc_ref, sem):
    fetch_maps(pos_ref, (p0, p1, p2, p3, p4), maps_ref, sem)
    consts = constants()

    def prep(i, _):
        for j in range(PREP):
            prepare(i * PREP + j, in_ref, maps_ref, rate_ref, consts, mat_ref, turn_ref, e_ref, g_ref, s_ref, m_ref)
        return 0

    lax.fori_loop(0, GROUPS // PREP, prep, 0)
    back_ref[...] = jnp.zeros((N, 256), F32)
    acc_ref[...] = jnp.zeros((2, 8, 128), F32)

    def step(i, _):
        groups = [GROUPS - 1 - (i * PAIRED + j) for j in range(PAIRED)]
        values = [sum_ref[c].astype(F32) for c in groups]
        turned = []
        for c, v in zip(groups, values):
            ev = e_ref[c] * v
            turned.append(jnp.concatenate([ev.astype(BF16), (ev * s_ref[c]).astype(BF16)], axis=1))
        local = [dot(turn_ref[c], x) for c, x in zip(groups, turned)]
        back, tangent = back_ref[:, :128], back_ref[:, 128:]
        states = []
        for j, c in enumerate(groups):
            tangent = tangent + s_ref[c, Q - 1 : Q, :] * back
            states.append(jnp.concatenate([back.astype(BF16), tangent.astype(BF16)], axis=1))
            scale = m_ref[c, 0:1, :] * m_ref[jnp.maximum(c - 1, 0), 0:1, :]
            back = scale * (back + local[j][:, :128])
            tangent = scale * (tangent + local[j][:, 128:])
        back_ref[:, :128] = back
        back_ref[:, 128:] = tangent
        mixed = [dot(mat_ref[c], jnp.concatenate([x, b], axis=0)) for c, x, b in zip(groups, turned, states)]
        rate_sum, skip_sum = acc_ref[0], acc_ref[1]
        for c, v, r in zip(groups, values, mixed):
            z = in_ref[c, Q + EXTRA :, :].astype(F32)
            change = g_ref[c] * (r[:, 128:] - s_ref[c] * r[:, :128])
            rate_sum = rate_sum + jnp.sum((z * change).reshape(16, 8, 128), axis=0)
            skip_sum = skip_sum + jnp.sum((z * v).reshape(16, 8, 128), axis=0)
        acc_ref[0] = rate_sum
        acc_ref[1] = skip_sum
        return 0

    lax.fori_loop(0, GROUPS // PAIRED, step, 0)
    lane = lax.broadcasted_iota(jnp.int32, (8, 128), 1)
    first = (pos_ref[0] * NZ + pos_ref[1]) * 2
    result = jnp.zeros((8, 128), F32)
    for kind in range(2):
        for head in range(2):
            picked = jnp.where((lane >= HEAD) if head else (lane < HEAD), acc_ref[kind], 0.0)
            value = jnp.sum(picked, keepdims=True)
            value = -value if kind == 0 else value
            result = jnp.where(lane == kind * H + first + head, value, result)
    out_ref[...] = result


def table_scratch(with_sums):
    square = pltpu.VMEM((GROUPS, Q, 128), F32)
    return [
        pltpu.VMEM((GROUPS, 2 * N, 128), BF16),
        pltpu.VMEM((GROUPS, Q, 256), BF16),
        pltpu.VMEM((GROUPS, N, Q), BF16),
        square,
        square,
        *([square] if with_sums else []),
        pltpu.VMEM((GROUPS, 8, 128), F32),
    ]


def series(pos, rows, pieces, rate):
    return pl.pallas_call(
        series_kernel,
        grid=(1,),
        in_specs=[SMEM, full((GROUPS, Q + EXTRA, 128)), HBM, HBM, HBM, HBM, HBM, full(rate.shape)],
        out_specs=full((GROUPS, Q, 128)),
        out_shape=jax.ShapeDtypeStruct((GROUPS, Q, 128), BF16),
        scratch_shapes=[
            *table_scratch(False),
            pltpu.VMEM((GROUPS, Q, 128), BF16),
            pltpu.VMEM((GROUPS, Q, 128), F32),
            pltpu.VMEM((N, 128), F32),
            pltpu.SemaphoreType.DMA,
        ],
        name="series",
        cost_estimate=pl.CostEstimate(flops=3_000_000_000, transcendentals=1_000_000, bytes_accessed=5_000_000),
    )(pos, rows, *pieces, rate)


def rates(pos, rows, summed, pieces, rate):
    return pl.pallas_call(
        rate_kernel,
        in_specs=[SMEM, full(rows.shape), full(summed.shape), HBM, HBM, HBM, HBM, HBM, full(rate.shape)],
        out_specs=full((8, 128)),
        out_shape=jax.ShapeDtypeStruct((8, 128), F32),
        scratch_shapes=[
            *table_scratch(True),
            pltpu.VMEM((N, 256), F32),
            pltpu.VMEM((2, 8, 128), F32),
            pltpu.SemaphoreType.DMA,
        ],
        name="rates",
        cost_estimate=pl.CostEstimate(flops=2_000_000_000, transcendentals=1_000_000, bytes_accessed=5_000_000),
    )(pos, rows, summed, *pieces, rate)


def gather_line(input_map, output_map):
    own = jnp.concatenate([input_map, output_map], axis=0)[None]
    last, after = shifted(own, "seq_1", 1), shifted(own, "seq_1", -1)
    far_last = shifted(jnp.concatenate([last, own]), "seq_1", 2)
    far_after = shifted(jnp.concatenate([own, after]), "seq_1", -2)
    far = shifted(own, "seq_1", 4)
    return jnp.concatenate([own, after, far_after, far, far_last, last])


def gather_plane(line):
    from_next = shifted(line, "seq_0", -1)
    from_last = shifted(line, "seq_0", 1)
    low = shifted(from_last[:4], "seq_0", 1)
    high = shifted(from_next[4:], "seq_0", -1)
    return line, from_next, from_last, low, high


def inner(cotangent, fixed_point, input_map, output_map, step_size, forget, decay_rate, skip_gain):
    my_y, my_z = lax.axis_index("seq_0"), lax.axis_index("seq_1")
    pos = jnp.stack([my_y, my_z]).astype(jnp.int32)
    first = (my_y * NZ + my_z) * 2
    own = jnp.stack([lax.dynamic_slice_in_dim(a, first, 2) for a in (decay_rate, skip_gain)])
    rate = jnp.repeat(own, HEAD, axis=1)

    line = gather_line(input_map[0], output_map[0])
    packed = pack(cotangent[0], fixed_point[0], step_size[0], forget)
    pieces = gather_plane(line)
    rows = lax.all_to_all(packed, SEQ, split_axis=0, concat_axis=0, tiled=True)
    summed = series(pos, rows, pieces, rate)
    result = lax.all_to_all(summed, SEQ, split_axis=0, concat_axis=0, tiled=True)
    totals = rates(pos, rows, summed, pieces, rate)
    for axis in BATCH:
        bit = 1
        while bit < lax.axis_size(axis):
            totals = totals + swapped(totals, axis, bit)
            bit *= 2
    copies = jnp.broadcast_to(totals[:1], (GROUPS, 1, 128))
    totals = lax.all_to_all(copies, SEQ, split_axis=0, concat_axis=0, tiled=True)
    totals = jnp.sum(totals, axis=(0, 1)) * (1.0 / (lax.axis_size(BATCH) * Q * GROUPS))
    return join(result)[None], totals[:H], totals[H:]


def solution(mesh):
    torus = Mesh(mesh.devices.reshape(4, 2, 4, 8), ("batch_0", "batch_1", "seq_0", "seq_1"))
    return jax.shard_map(
        inner,
        mesh=torus,
        in_specs=(
            P(BATCH, SEQ, None),
            P(BATCH, SEQ, None),
            P(BATCH, SEQ, None),
            P(BATCH, SEQ, None),
            P(BATCH, None, SEQ),
            P(BATCH, SEQ),
            P(),
            P(),
        ),
        out_specs=(P(BATCH, SEQ, None), P(), P()),
        check_vma=False,
    )
```

```python
import jax
import jax.numpy as jnp
from jax import lax
from jax.experimental import pallas as pl
from jax.experimental.pallas import tpu as pltpu
from jax.sharding import Mesh
from jax.sharding import PartitionSpec as P

H = 64
HEAD = 64
N = 128
Q = 128
EXTRA = 8
GROUPS = 32
NY = 4
NZ = 8
UNROLL = 16
PREP = 16
PAIRED = 8
SEQ = ("seq_0", "seq_1")
BATCH = ("batch_0", "batch_1")
F32 = jnp.float32
BF16 = jnp.bfloat16


def shifted(x, axis, by):
    size = lax.axis_size(axis)
    return lax.ppermute(x, axis, [(i, (i + by) % size) for i in range(size)])


def swapped(x, axis, bit):
    size = lax.axis_size(axis)
    return lax.ppermute(x, axis, [(i, i ^ bit) for i in range(size)])


def full(shape):
    return pl.BlockSpec(shape, lambda *_: (0,) * len(shape))


HBM = pl.BlockSpec(memory_space=pltpu.HBM)
SMEM = pl.BlockSpec(memory_space=pltpu.SMEM)


def halves(x):
    high = x.astype(BF16)
    return high, (x - high.astype(F32)).astype(BF16)


def pack_kernel(step_ref, forget_ref, cot_ref, fixed_ref, out_ref, sem):
    copies = []
    for j in range(GROUPS):
        lanes = pl.ds(j * 128, 128)
        copies.append(pltpu.make_async_copy(cot_ref.at[:, lanes], out_ref.at[j, pl.ds(0, Q), :], sem))
        copies.append(pltpu.make_async_copy(fixed_ref.at[:, lanes], out_ref.at[j, pl.ds(Q + EXTRA, Q), :], sem))
    for c in copies:
        c.start()
    step_high, step_low = halves(step_ref[...])
    step_high, step_low = step_high.astype(F32), step_low.astype(F32)
    tail = [f.astype(F32) for f in halves(forget_ref[...])] + [jnp.zeros((2, Q), F32)]
    for j in range(GROUPS):
        two = slice(2 * j, 2 * j + 2)
        rows = jnp.concatenate([step_high[two], step_low[two], *tail], axis=0)
        out_ref[j, Q : Q + EXTRA, :] = rows.astype(BF16)
    for c in copies:
        c.wait()


def pack(cot, fixed, step, forget):
    shape = (GROUPS, 2 * Q + EXTRA, 128)
    return pl.pallas_call(
        pack_kernel,
        in_specs=[full(step.shape), full(forget.shape), HBM, HBM],
        out_specs=full(shape),
        out_shape=jax.ShapeDtypeStruct(shape, BF16),
        scratch_shapes=[pltpu.SemaphoreType.DMA],
        name="pack",
    )(step, forget, cot, fixed)


def join_kernel(in_ref, out_ref, sem):
    copies = [
        pltpu.make_async_copy(in_ref.at[j], out_ref.at[:, pl.ds(j * 128, 128)], sem) for j in range(GROUPS)
    ]
    for c in copies:
        c.start()
    for c in copies:
        c.wait()


def join(x):
    return pl.pallas_call(
        join_kernel,
        in_specs=[full(x.shape)],
        out_specs=HBM,
        out_shape=jax.ShapeDtypeStruct((Q, GROUPS * 128), BF16),
        scratch_shapes=[pltpu.SemaphoreType.DMA],
        name="join",
    )(x)


def dot(a, b):
    return lax.dot_general(a, b, (((1,), (0,)), ((), ())), preferred_element_type=F32)


def dot_t(a, b):
    return lax.dot_general(a, b, (((1,), (1,)), ((), ())), preferred_element_type=F32)


def fetch_maps(pos_ref, pieces, maps_ref, sem):
    my_y, my_z = pos_ref[0], pos_ref[1]
    copies = []
    for dy in range(NY):
        for dz in range(NZ):
            if dy == 0:
                source = pieces[0].at[dz]
            elif dy == 1:
                source = pieces[1].at[dz]
            elif dy == 3:
                source = pieces[2].at[dz]
            else:
                source = pieces[3].at[dz] if dz < 4 else pieces[4].at[dz - 4]
            place = ((my_y + dy) % NY) * NZ + (my_z + dz) % NZ
            copies.append(pltpu.make_async_copy(source, maps_ref.at[place], sem))
    for c in copies:
        c.start()
    for c in copies:
        c.wait()


def constants():
    rows = lax.broadcasted_iota(jnp.int32, (Q, Q), 0)
    cols = lax.broadcasted_iota(jnp.int32, (Q, Q), 1)
    lower = (rows >= cols).astype(F32).astype(BF16)
    same = (rows == cols).astype(F32).astype(BF16)
    return rows <= cols, lower, same


def tables_kernel(pos_ref, p0, p1, p2, p3, p4, mat_ref, turn_ref, maps_ref, sem):
    fetch_maps(pos_ref, (p0, p1, p2, p3, p4), maps_ref, sem)
    upper, _, same = constants()

    def step(i, _):
        for j in range(PREP):
            c = i * PREP + j
            both = maps_ref[c]
            b_rows, c_rows = both[:N], both[N:]
            prod = dot_t(jnp.concatenate([b_rows, same], axis=0), c_rows)
            mat_ref[c, :, :N] = jnp.where(upper, prod[:Q], 0.0).astype(BF16)
            mat_ref[c, :, N:] = b_rows
            turn_ref[c] = prod[Q:].astype(BF16)
        return 0

    lax.fori_loop(0, GROUPS // PREP, step, 0)


def tables(pos, pieces):
    shapes = ((GROUPS, Q, 256), (GROUPS, N, Q))
    return pl.pallas_call(
        tables_kernel,
        in_specs=[SMEM, HBM, HBM, HBM, HBM, HBM],
        out_specs=[full(shape) for shape in shapes],
        out_shape=[jax.ShapeDtypeStruct(shape, BF16) for shape in shapes],
        scratch_shapes=[pltpu.VMEM((GROUPS, 2 * N, 128), BF16), pltpu.SemaphoreType.DMA],
        name="tables",
        cost_estimate=pl.CostEstimate(flops=300_000_000, transcendentals=0, bytes_accessed=5_000_000),
    )(pos, *pieces)


def prepare(c, in_ref, rate_ref, consts, e_ref, g_ref, s_ref, m_ref):
    _, lower, same = consts
    rows = in_ref[c, Q : Q + EXTRA, :].astype(F32)

    def wide(first, second):
        return jnp.concatenate(
            [jnp.broadcast_to(rows[first : first + 1], (HEAD, Q)), jnp.broadcast_to(rows[second : second + 1], (HEAD, Q))],
            axis=0,
        ).astype(BF16)

    steps = jnp.concatenate([wide(0, 1), wide(2, 3)], axis=1)
    forgets = jnp.concatenate([wide(4, 4), wide(5, 5)], axis=1)
    lower_twice = jnp.concatenate([lower, lower], axis=1)
    same_twice = jnp.concatenate([same, same], axis=1)
    sums = dot_t(jnp.concatenate([lower_twice, same_twice], axis=0), steps)
    step_sum, step_col = sums[:Q], sums[Q:]
    forget_sum = dot_t(lower_twice, forgets)
    log_decay = -(rate_ref[0:1, :] * step_sum + forget_sum)
    middle = 0.5 * log_decay[Q - 1 : Q, :]
    gap = log_decay - middle
    e_ref[c] = jnp.exp(gap)
    g_ref[c] = step_col * jnp.exp(-gap)
    if s_ref is not None:
        s_ref[c] = step_sum
    m_ref[c] = jnp.broadcast_to(jnp.exp(middle), (8, 128))


def series_kernel(in_ref, mat_ref, turn_ref, rate_ref, out_ref, e_ref, g_ref, m_ref, v_ref, sum_ref, back_ref):
    consts = constants()

    def prep(i, _):
        for j in range(PREP):
            prepare(i * PREP + j, in_ref, rate_ref, consts, e_ref, g_ref, None, m_ref)
        return 0

    lax.fori_loop(0, GROUPS // PREP, prep, 0)
    skip = rate_ref[1:2, :]
    for k in range(3):
        back_ref[...] = jnp.zeros((N, 128), F32)

        def step(i, _):
            groups = [GROUPS - 1 - (i * UNROLL + j) for j in range(UNROLL)]
            values = [(in_ref[c, :Q, :] if k == 0 else v_ref[c]).astype(F32) for c in groups]
            turned = [(e_ref[c] * v).astype(BF16) for c, v in zip(groups, values)]
            local = [dot(turn_ref[c], x) for c, x in zip(groups, turned)]
            back = back_ref[...]
            states = []
            for j, c in enumerate(groups):
                states.append(back.astype(BF16))
                scale = m_ref[c, 0:1, :] * m_ref[jnp.maximum(c - 1, 0), 0:1, :]
                back = scale * (back + local[j])
            back_ref[...] = back
            mixed = [
                dot(mat_ref[c], jnp.concatenate([x, b], axis=0)) for c, x, b in zip(groups, turned, states)
            ]
            fresh = [
                (g_ref[c] * r + skip * v).astype(BF16) for c, r, v in zip(groups, mixed, values)
            ]
            totals = [
                (v if k == 0 else sum_ref[c]) + n.astype(F32) for c, v, n in zip(groups, values, fresh)
            ]
            for c, n, t in zip(groups, fresh, totals):
                if k < 2:
                    v_ref[c] = n
                    sum_ref[c] = t
                else:
                    out_ref[c] = t.astype(BF16)
            return 0

        lax.fori_loop(0, GROUPS // UNROLL, step, 0)


def rate_kernel(pos_ref, in_ref, sum_ref, mat_ref, turn_ref, rate_ref, out_ref, e_ref, g_ref, s_ref, m_ref, back_ref, acc_ref):
    consts = constants()

    def prep(i, _):
        for j in range(PREP):
            prepare(i * PREP + j, in_ref, rate_ref, consts, e_ref, g_ref, s_ref, m_ref)
        return 0

    lax.fori_loop(0, GROUPS // PREP, prep, 0)
    back_ref[...] = jnp.zeros((N, 256), F32)
    acc_ref[...] = jnp.zeros((2, 8, 128), F32)

    def step(i, _):
        groups = [GROUPS - 1 - (i * PAIRED + j) for j in range(PAIRED)]
        values = [sum_ref[c].astype(F32) for c in groups]
        turned = []
        for c, v in zip(groups, values):
            ev = e_ref[c] * v
            turned.append(jnp.concatenate([ev.astype(BF16), (ev * s_ref[c]).astype(BF16)], axis=1))
        local = [dot(turn_ref[c], x) for c, x in zip(groups, turned)]
        back, tangent = back_ref[:, :128], back_ref[:, 128:]
        states = []
        for j, c in enumerate(groups):
            tangent = tangent + s_ref[c, Q - 1 : Q, :] * back
            states.append(jnp.concatenate([back.astype(BF16), tangent.astype(BF16)], axis=1))
            scale = m_ref[c, 0:1, :] * m_ref[jnp.maximum(c - 1, 0), 0:1, :]
            back = scale * (back + local[j][:, :128])
            tangent = scale * (tangent + local[j][:, 128:])
        back_ref[:, :128] = back
        back_ref[:, 128:] = tangent
        mixed = [dot(mat_ref[c], jnp.concatenate([x, b], axis=0)) for c, x, b in zip(groups, turned, states)]
        rate_sum, skip_sum = acc_ref[0], acc_ref[1]
        for c, v, r in zip(groups, values, mixed):
            z = in_ref[c, Q + EXTRA :, :].astype(F32)
            change = g_ref[c] * (r[:, 128:] - s_ref[c] * r[:, :128])
            rate_sum = rate_sum + jnp.sum((z * change).reshape(16, 8, 128), axis=0)
            skip_sum = skip_sum + jnp.sum((z * v).reshape(16, 8, 128), axis=0)
        acc_ref[0] = rate_sum
        acc_ref[1] = skip_sum
        return 0

    lax.fori_loop(0, GROUPS // PAIRED, step, 0)
    lane = lax.broadcasted_iota(jnp.int32, (8, 128), 1)
    first = (pos_ref[0] * NZ + pos_ref[1]) * 2
    result = jnp.zeros((8, 128), F32)
    for kind in range(2):
        for head in range(2):
            picked = jnp.where((lane >= HEAD) if head else (lane < HEAD), acc_ref[kind], 0.0)
            value = jnp.sum(picked, keepdims=True)
            value = -value if kind == 0 else value
            result = jnp.where(lane == kind * H + first + head, value, result)
    out_ref[...] = result


def decay_scratch(with_sums):
    square = pltpu.VMEM((GROUPS, Q, 128), F32)
    return [*[square] * (3 if with_sums else 2), pltpu.VMEM((GROUPS, 8, 128), F32)]


def series(rows, mat, turn, rate):
    return pl.pallas_call(
        series_kernel,
        in_specs=[full(rows.shape), full(mat.shape), full(turn.shape), full(rate.shape)],
        out_specs=full((GROUPS, Q, 128)),
        out_shape=jax.ShapeDtypeStruct((GROUPS, Q, 128), BF16),
        scratch_shapes=[
            *decay_scratch(False),
            pltpu.VMEM((GROUPS, Q, 128), BF16),
            pltpu.VMEM((GROUPS, Q, 128), F32),
            pltpu.VMEM((N, 128), F32),
        ],
        name="series",
        cost_estimate=pl.CostEstimate(flops=3_000_000_000, transcendentals=1_000_000, bytes_accessed=5_000_000),
    )(rows, mat, turn, rate)


def rates(pos, rows, summed, mat, turn, rate):
    return pl.pallas_call(
        rate_kernel,
        in_specs=[SMEM, full(rows.shape), full(summed.shape), full(mat.shape), full(turn.shape), full(rate.shape)],
        out_specs=full((8, 128)),
        out_shape=jax.ShapeDtypeStruct((8, 128), F32),
        scratch_shapes=[*decay_scratch(True), pltpu.VMEM((N, 256), F32), pltpu.VMEM((2, 8, 128), F32)],
        name="rates",
        cost_estimate=pl.CostEstimate(flops=2_000_000_000, transcendentals=1_000_000, bytes_accessed=5_000_000),
    )(pos, rows, summed, mat, turn, rate)


def gather_line(input_map, output_map):
    own = jnp.concatenate([input_map, output_map], axis=0)[None]
    last, after = shifted(own, "seq_1", 1), shifted(own, "seq_1", -1)
    far_last = shifted(jnp.concatenate([last, own, after]), "seq_1", 3)
    far_after = shifted(jnp.concatenate([last, own]), "seq_1", -3)
    return jnp.concatenate([own, after, far_after, far_last, last])


def gather_plane(line):
    from_next = shifted(line, "seq_0", -1)
    from_last = shifted(line, "seq_0", 1)
    low = shifted(from_last[:4], "seq_0", 1)
    high = shifted(from_next[4:], "seq_0", -1)
    return line, from_next, from_last, low, high


def inner(cotangent, fixed_point, input_map, output_map, step_size, forget, decay_rate, skip_gain):
    my_y, my_z = lax.axis_index("seq_0"), lax.axis_index("seq_1")
    pos = jnp.stack([my_y, my_z]).astype(jnp.int32)
    first = (my_y * NZ + my_z) * 2
    own = jnp.stack([lax.dynamic_slice_in_dim(a, first, 2) for a in (decay_rate, skip_gain)])
    rate = jnp.repeat(own, HEAD, axis=1)

    line = gather_line(input_map[0], output_map[0])
    packed = pack(cotangent[0], fixed_point[0], step_size[0], forget)
    pieces = gather_plane(line)
    rows = lax.all_to_all(packed, SEQ, split_axis=0, concat_axis=0, tiled=True)
    mat, turn = tables(pos, pieces)
    summed = series(rows, mat, turn, rate)
    result = lax.all_to_all(summed, SEQ, split_axis=0, concat_axis=0, tiled=True)
    totals = rates(pos, rows, summed, mat, turn, rate)
    for axis in BATCH:
        bit = 1
        while bit < lax.axis_size(axis):
            totals = totals + swapped(totals, axis, bit)
            bit *= 2
    copies = jnp.broadcast_to(totals[:1], (GROUPS, 1, 128))
    totals = lax.all_to_all(copies, SEQ, split_axis=0, concat_axis=0, tiled=True)
    totals = jnp.sum(totals, axis=(0, 1)) * (1.0 / (lax.axis_size(BATCH) * Q * GROUPS))
    return join(result)[None], totals[:H], totals[H:]


def solution(mesh):
    torus = Mesh(mesh.devices.reshape(4, 2, 4, 8), ("batch_0", "batch_1", "seq_0", "seq_1"))
    return jax.shard_map(
        inner,
        mesh=torus,
        in_specs=(
            P(BATCH, SEQ, None),
            P(BATCH, SEQ, None),
            P(BATCH, SEQ, None),
            P(BATCH, SEQ, None),
            P(BATCH, None, SEQ),
            P(BATCH, SEQ),
            P(),
            P(),
        ),
        out_specs=(P(BATCH, SEQ, None), P(), P()),
        check_vma=False,
    )
```

```python
import jax
import jax.numpy as jnp
from jax import lax
from jax.experimental import pallas as pl
from jax.experimental.pallas import tpu as pltpu
from jax.sharding import Mesh
from jax.sharding import PartitionSpec as P

H = 64
HEAD = 64
N = 128
Q = 128
EXTRA = 8
GROUPS = 32
NY = 4
NZ = 8
UNROLL = 16
PREP = 16
PAIRED = 8
SEQ = ("seq_0", "seq_1")
BATCH = ("batch_0", "batch_1")
F32 = jnp.float32
BF16 = jnp.bfloat16


def shifted(x, axis, by):
    size = lax.axis_size(axis)
    return lax.ppermute(x, axis, [(i, (i + by) % size) for i in range(size)])


def swapped(x, axis, bit):
    size = lax.axis_size(axis)
    return lax.ppermute(x, axis, [(i, i ^ bit) for i in range(size)])


def full(shape):
    return pl.BlockSpec(shape, lambda *_: (0,) * len(shape))


HBM = pl.BlockSpec(memory_space=pltpu.HBM)
SMEM = pl.BlockSpec(memory_space=pltpu.SMEM)


def halves(x):
    high = x.astype(BF16)
    return high, (x - high.astype(F32)).astype(BF16)


def pack_kernel(step_ref, forget_ref, cot_ref, fixed_ref, out_ref, rows_ref, in_sems, out_sems):
    chunks = []
    for i in range(4):
        copies = []
        for j in range(8 * i, 8 * i + 8):
            lanes = pl.ds(j * 128, 128)
            copies.append(pltpu.make_async_copy(cot_ref.at[:, lanes], rows_ref.at[j, pl.ds(0, Q), :], in_sems.at[i]))
            copies.append(
                pltpu.make_async_copy(fixed_ref.at[:, lanes], rows_ref.at[j, pl.ds(Q + EXTRA, Q), :], in_sems.at[i])
            )
        chunks.append(copies)
    for copies in chunks:
        for c in copies:
            c.start()
    step_high, step_low = halves(step_ref[...])
    step_high, step_low = step_high.astype(F32), step_low.astype(F32)
    tail = [f.astype(F32) for f in halves(forget_ref[...])] + [jnp.zeros((2, Q), F32)]
    for j in range(GROUPS):
        two = slice(2 * j, 2 * j + 2)
        rows = jnp.concatenate([step_high[two], step_low[two], *tail], axis=0)
        rows_ref[j, Q : Q + EXTRA, :] = rows.astype(BF16)
    results = []
    for i, copies in enumerate(chunks):
        for c in copies:
            c.wait()
        part = pl.ds(8 * i, 8)
        results.append(pltpu.make_async_copy(rows_ref.at[part], out_ref.at[part], out_sems.at[i]))
        results[-1].start()
    for r in results:
        r.wait()


def pack(cot, fixed, step, forget):
    shape = (GROUPS, 2 * Q + EXTRA, 128)
    return pl.pallas_call(
        pack_kernel,
        in_specs=[full(step.shape), full(forget.shape), HBM, HBM],
        out_specs=HBM,
        out_shape=jax.ShapeDtypeStruct(shape, BF16),
        scratch_shapes=[
            pltpu.VMEM(shape, BF16),
            pltpu.SemaphoreType.DMA((4,)),
            pltpu.SemaphoreType.DMA((4,)),
        ],
        name="pack",
    )(step, forget, cot, fixed)


def join_kernel(in_ref, out_ref, sem):
    copies = [
        pltpu.make_async_copy(in_ref.at[j], out_ref.at[:, pl.ds(j * 128, 128)], sem) for j in range(GROUPS)
    ]
    for c in copies:
        c.start()
    for c in copies:
        c.wait()


def join(x):
    return pl.pallas_call(
        join_kernel,
        in_specs=[full(x.shape)],
        out_specs=HBM,
        out_shape=jax.ShapeDtypeStruct((Q, GROUPS * 128), BF16),
        scratch_shapes=[pltpu.SemaphoreType.DMA],
        name="join",
    )(x)


def dot(a, b):
    return lax.dot_general(a, b, (((1,), (0,)), ((), ())), preferred_element_type=F32)


def dot_t(a, b):
    return lax.dot_general(a, b, (((1,), (1,)), ((), ())), preferred_element_type=F32)


def fetch_maps(pos_ref, pieces, maps_ref, sem):
    my_y, my_z = pos_ref[0], pos_ref[1]
    copies = []
    for dy in range(NY):
        for dz in range(NZ):
            if dy == 0:
                source = pieces[0].at[dz]
            elif dy == 1:
                source = pieces[1].at[dz]
            elif dy == 3:
                source = pieces[2].at[dz]
            else:
                source = pieces[3].at[dz] if dz < 4 else pieces[4].at[dz - 4]
            place = ((my_y + dy) % NY) * NZ + (my_z + dz) % NZ
            copies.append(pltpu.make_async_copy(source, maps_ref.at[place], sem))
    for c in copies:
        c.start()
    for c in copies:
        c.wait()


def constants():
    rows = lax.broadcasted_iota(jnp.int32, (Q, Q), 0)
    cols = lax.broadcasted_iota(jnp.int32, (Q, Q), 1)
    lower = (rows >= cols).astype(F32).astype(BF16)
    same = (rows == cols).astype(F32).astype(BF16)
    return rows <= cols, lower, same


def prepare(c, in_ref, maps_ref, rate_ref, consts, mat_ref, turn_ref, e_ref, g_ref, s_ref, m_ref):
    upper, lower, same = consts
    both = maps_ref[c]
    b_rows, c_rows = both[:N], both[N:]
    prod = dot_t(jnp.concatenate([b_rows, same], axis=0), c_rows)
    mat_ref[c, :, :N] = jnp.where(upper, prod[:Q], 0.0).astype(BF16)
    mat_ref[c, :, N:] = b_rows
    turn_ref[c] = prod[Q:].astype(BF16)
    rows = in_ref[c, Q : Q + EXTRA, :].astype(F32)

    def wide(first, second):
        return jnp.concatenate(
            [jnp.broadcast_to(rows[first : first + 1], (HEAD, Q)), jnp.broadcast_to(rows[second : second + 1], (HEAD, Q))],
            axis=0,
        ).astype(BF16)

    steps = jnp.concatenate([wide(0, 1), wide(2, 3)], axis=1)
    forgets = jnp.concatenate([wide(4, 4), wide(5, 5)], axis=1)
    lower_twice = jnp.concatenate([lower, lower], axis=1)
    same_twice = jnp.concatenate([same, same], axis=1)
    sums = dot_t(
        jnp.concatenate([lower_twice, same_twice], axis=0), jnp.concatenate([steps, forgets], axis=0)
    )
    step_sum, step_col, forget_sum = sums[:Q, :128], sums[Q:, :128], sums[:Q, 128:]
    log_decay = -(rate_ref[0:1, :] * step_sum + forget_sum)
    middle = 0.5 * log_decay[Q - 1 : Q, :]
    gap = log_decay - middle
    e_ref[c] = jnp.exp(gap)
    g_ref[c] = step_col * jnp.exp(-gap)
    if s_ref is not None:
        s_ref[c] = step_sum
    m_ref[c] = jnp.broadcast_to(jnp.exp(middle), (8, 128))


def series_kernel(pos_ref, in_ref, p0, p1, p2, p3, p4, rate_ref, out_ref, maps_ref, mat_ref, turn_ref, e_ref, g_ref, m_ref, v_ref, sum_ref, back_ref, sem):
    fetch_maps(pos_ref, (p0, p1, p2, p3, p4), maps_ref, sem)
    consts = constants()

    def prep(i, _):
        for j in range(PREP):
            prepare(i * PREP + j, in_ref, maps_ref, rate_ref, consts, mat_ref, turn_ref, e_ref, g_ref, None, m_ref)
        return 0

    lax.fori_loop(0, GROUPS // PREP, prep, 0)
    skip = rate_ref[1:2, :]
    for k in range(3):
        back_ref[...] = jnp.zeros((N, 128), F32)

        def step(i, _):
            groups = [GROUPS - 1 - (i * UNROLL + j) for j in range(UNROLL)]
            values = [(in_ref[c, :Q, :] if k == 0 else v_ref[c]).astype(F32) for c in groups]
            turned = [(e_ref[c] * v).astype(BF16) for c, v in zip(groups, values)]
            local = [dot(turn_ref[c], x) for c, x in zip(groups, turned)]
            back = back_ref[...]
            states = []
            for j, c in enumerate(groups):
                states.append(back.astype(BF16))
                scale = m_ref[c, 0:1, :] * m_ref[jnp.maximum(c - 1, 0), 0:1, :]
                back = scale * (back + local[j])
            back_ref[...] = back
            mixed = [
                dot(mat_ref[c], jnp.concatenate([x, b], axis=0)) for c, x, b in zip(groups, turned, states)
            ]
            fresh = [
                (g_ref[c] * r + skip * v).astype(BF16) for c, r, v in zip(groups, mixed, values)
            ]
            totals = [
                (v if k == 0 else sum_ref[c]) + n.astype(F32) for c, v, n in zip(groups, values, fresh)
            ]
            for c, n, t in zip(groups, fresh, totals):
                if k < 2:
                    v_ref[c] = n
                    sum_ref[c] = t
                else:
                    out_ref[c] = t.astype(BF16)
            return 0

        lax.fori_loop(0, GROUPS // UNROLL, step, 0)


def rate_kernel(pos_ref, in_ref, sum_ref, p0, p1, p2, p3, p4, rate_ref, out_ref, maps_ref, mat_ref, turn_ref, e_ref, g_ref, s_ref, m_ref, back_ref, acc_ref, sem):
    fetch_maps(pos_ref, (p0, p1, p2, p3, p4), maps_ref, sem)
    consts = constants()

    def prep(i, _):
        for j in range(PREP):
            prepare(i * PREP + j, in_ref, maps_ref, rate_ref, consts, mat_ref, turn_ref, e_ref, g_ref, s_ref, m_ref)
        return 0

    lax.fori_loop(0, GROUPS // PREP, prep, 0)
    back_ref[...] = jnp.zeros((N, 256), F32)
    acc_ref[...] = jnp.zeros((2, 8, 128), F32)

    def step(i, _):
        groups = [GROUPS - 1 - (i * PAIRED + j) for j in range(PAIRED)]
        values = [sum_ref[c].astype(F32) for c in groups]
        turned = []
        for c, v in zip(groups, values):
            ev = e_ref[c] * v
            turned.append(jnp.concatenate([ev.astype(BF16), (ev * s_ref[c]).astype(BF16)], axis=1))
        local = [dot(turn_ref[c], x) for c, x in zip(groups, turned)]
        back, tangent = back_ref[:, :128], back_ref[:, 128:]
        states = []
        for j, c in enumerate(groups):
            tangent = tangent + s_ref[c, Q - 1 : Q, :] * back
            states.append(jnp.concatenate([back.astype(BF16), tangent.astype(BF16)], axis=1))
            scale = m_ref[c, 0:1, :] * m_ref[jnp.maximum(c - 1, 0), 0:1, :]
            back = scale * (back + local[j][:, :128])
            tangent = scale * (tangent + local[j][:, 128:])
        back_ref[:, :128] = back
        back_ref[:, 128:] = tangent
        mixed = [dot(mat_ref[c], jnp.concatenate([x, b], axis=0)) for c, x, b in zip(groups, turned, states)]
        rate_sum, skip_sum = acc_ref[0], acc_ref[1]
        for c, v, r in zip(groups, values, mixed):
            z = in_ref[c, Q + EXTRA :, :].astype(F32)
            change = g_ref[c] * (r[:, 128:] - s_ref[c] * r[:, :128])
            rate_sum = rate_sum + jnp.sum((z * change).reshape(16, 8, 128), axis=0)
            skip_sum = skip_sum + jnp.sum((z * v).reshape(16, 8, 128), axis=0)
        acc_ref[0] = rate_sum
        acc_ref[1] = skip_sum
        return 0

    lax.fori_loop(0, GROUPS // PAIRED, step, 0)
    lane = lax.broadcasted_iota(jnp.int32, (8, 128), 1)
    first = (pos_ref[0] * NZ + pos_ref[1]) * 2
    result = jnp.zeros((8, 128), F32)
    for kind in range(2):
        for head in range(2):
            picked = jnp.where((lane >= HEAD) if head else (lane < HEAD), acc_ref[kind], 0.0)
            value = jnp.sum(picked, keepdims=True)
            value = -value if kind == 0 else value
            result = jnp.where(lane == kind * H + first + head, value, result)
    out_ref[...] = result


def table_scratch(with_sums):
    square = pltpu.VMEM((GROUPS, Q, 128), F32)
    return [
        pltpu.VMEM((GROUPS, 2 * N, 128), BF16),
        pltpu.VMEM((GROUPS, Q, 256), BF16),
        pltpu.VMEM((GROUPS, N, Q), BF16),
        square,
        square,
        *([square] if with_sums else []),
        pltpu.VMEM((GROUPS, 8, 128), F32),
    ]


def series(pos, rows, pieces, rate):
    return pl.pallas_call(
        series_kernel,
        grid=(1,),
        in_specs=[SMEM, full((GROUPS, Q + EXTRA, 128)), HBM, HBM, HBM, HBM, HBM, full(rate.shape)],
        out_specs=full((GROUPS, Q, 128)),
        out_shape=jax.ShapeDtypeStruct((GROUPS, Q, 128), BF16),
        scratch_shapes=[
            *table_scratch(False),
            pltpu.VMEM((GROUPS, Q, 128), BF16),
            pltpu.VMEM((GROUPS, Q, 128), F32),
            pltpu.VMEM((N, 128), F32),
            pltpu.SemaphoreType.DMA,
        ],
        name="series",
        cost_estimate=pl.CostEstimate(flops=3_000_000_000, transcendentals=1_000_000, bytes_accessed=5_000_000),
    )(pos, rows, *pieces, rate)


def rates(pos, rows, summed, pieces, rate):
    return pl.pallas_call(
        rate_kernel,
        in_specs=[SMEM, full(rows.shape), full(summed.shape), HBM, HBM, HBM, HBM, HBM, full(rate.shape)],
        out_specs=full((8, 128)),
        out_shape=jax.ShapeDtypeStruct((8, 128), F32),
        scratch_shapes=[
            *table_scratch(True),
            pltpu.VMEM((N, 256), F32),
            pltpu.VMEM((2, 8, 128), F32),
            pltpu.SemaphoreType.DMA,
        ],
        name="rates",
        cost_estimate=pl.CostEstimate(flops=2_000_000_000, transcendentals=1_000_000, bytes_accessed=5_000_000),
    )(pos, rows, summed, *pieces, rate)


def gather_line(input_map, output_map):
    own = jnp.concatenate([input_map, output_map], axis=0)[None]
    last, after = shifted(own, "seq_1", 1), shifted(own, "seq_1", -1)
    far_last = shifted(jnp.concatenate([last, own]), "seq_1", 2)
    far_after = shifted(jnp.concatenate([own, after]), "seq_1", -2)
    far = shifted(own, "seq_1", 4)
    return jnp.concatenate([own, after, far_after, far, far_last, last])


def gather_plane(line):
    from_next = shifted(line, "seq_0", -1)
    from_last = shifted(line, "seq_0", 1)
    low = shifted(from_last[:4], "seq_0", 1)
    high = shifted(from_next[4:], "seq_0", -1)
    return line, from_next, from_last, low, high


def inner(cotangent, fixed_point, input_map, output_map, step_size, forget, decay_rate, skip_gain):
    my_y, my_z = lax.axis_index("seq_0"), lax.axis_index("seq_1")
    pos = jnp.stack([my_y, my_z]).astype(jnp.int32)
    first = (my_y * NZ + my_z) * 2
    own = jnp.stack([lax.dynamic_slice_in_dim(a, first, 2) for a in (decay_rate, skip_gain)])
    rate = jnp.repeat(own, HEAD, axis=1)

    line = gather_line(input_map[0], output_map[0])
    packed = pack(cotangent[0], fixed_point[0], step_size[0], forget)
    pieces = gather_plane(line)
    rows = lax.all_to_all(packed, SEQ, split_axis=0, concat_axis=0, tiled=True)
    summed = series(pos, rows, pieces, rate)
    result = lax.all_to_all(summed, SEQ, split_axis=0, concat_axis=0, tiled=True)
    totals = rates(pos, rows, summed, pieces, rate)
    for axis in BATCH:
        bit = 1
        while bit < lax.axis_size(axis):
            totals = totals + swapped(totals, axis, bit)
            bit *= 2
    copies = jnp.broadcast_to(totals[:1], (GROUPS, 1, 128))
    totals = lax.all_to_all(copies, SEQ, split_axis=0, concat_axis=0, tiled=True)
    totals = jnp.sum(totals, axis=(0, 1)) * (1.0 / (lax.axis_size(BATCH) * Q * GROUPS))
    return join(result)[None], totals[:H], totals[H:]


def solution(mesh):
    torus = Mesh(mesh.devices.reshape(4, 2, 4, 8), ("batch_0", "batch_1", "seq_0", "seq_1"))
    return jax.shard_map(
        inner,
        mesh=torus,
        in_specs=(
            P(BATCH, SEQ, None),
            P(BATCH, SEQ, None),
            P(BATCH, SEQ, None),
            P(BATCH, SEQ, None),
            P(BATCH, None, SEQ),
            P(BATCH, SEQ),
            P(),
            P(),
        ),
        out_specs=(P(BATCH, SEQ, None), P(), P()),
        check_vma=False,
    )
```

```python
import jax
import jax.numpy as jnp
from jax import lax
from jax.experimental import pallas as pl
from jax.experimental.pallas import tpu as pltpu
from jax.sharding import Mesh
from jax.sharding import PartitionSpec as P

H = 64
HEAD = 64
N = 128
Q = 128
EXTRA = 8
GROUPS = 32
NY = 4
NZ = 8
UNROLL = 16
PREP = 16
PAIRED = 8
SEQ = ("seq_0", "seq_1")
BATCH = ("batch_0", "batch_1")
F32 = jnp.float32
BF16 = jnp.bfloat16


def shifted(x, axis, by):
    size = lax.axis_size(axis)
    return lax.ppermute(x, axis, [(i, (i + by) % size) for i in range(size)])


def swapped(x, axis, bit):
    size = lax.axis_size(axis)
    return lax.ppermute(x, axis, [(i, i ^ bit) for i in range(size)])


def full(shape):
    return pl.BlockSpec(shape, lambda *_: (0,) * len(shape))


HBM = pl.BlockSpec(memory_space=pltpu.HBM)
SMEM = pl.BlockSpec(memory_space=pltpu.SMEM)


def halves(x):
    high = x.astype(BF16)
    return high, (x - high.astype(F32)).astype(BF16)


def pack_kernel(step_ref, forget_ref, cot_ref, fixed_ref, out_ref, rows_ref, in_sems, out_sems):
    chunks = []
    for i in range(4):
        copies = []
        for j in range(8 * i, 8 * i + 8):
            lanes = pl.ds(j * 128, 128)
            copies.append(pltpu.make_async_copy(cot_ref.at[:, lanes], rows_ref.at[j, pl.ds(0, Q), :], in_sems.at[i]))
            copies.append(
                pltpu.make_async_copy(fixed_ref.at[:, lanes], rows_ref.at[j, pl.ds(Q + EXTRA, Q), :], in_sems.at[i])
            )
        chunks.append(copies)
    for copies in chunks:
        for c in copies:
            c.start()
    step_high, step_low = halves(step_ref[...])
    step_high, step_low = step_high.astype(F32), step_low.astype(F32)
    tail = [f.astype(F32) for f in halves(forget_ref[...])] + [jnp.zeros((2, Q), F32)]
    for j in range(GROUPS):
        two = slice(2 * j, 2 * j + 2)
        rows = jnp.concatenate([step_high[two], step_low[two], *tail], axis=0)
        rows_ref[j, Q : Q + EXTRA, :] = rows.astype(BF16)
    results = []
    for i, copies in enumerate(chunks):
        for c in copies:
            c.wait()
        part = pl.ds(8 * i, 8)
        results.append(pltpu.make_async_copy(rows_ref.at[part], out_ref.at[part], out_sems.at[i]))
        results[-1].start()
    for r in results:
        r.wait()


def pack(cot, fixed, step, forget):
    shape = (GROUPS, 2 * Q + EXTRA, 128)
    return pl.pallas_call(
        pack_kernel,
        in_specs=[full(step.shape), full(forget.shape), HBM, HBM],
        out_specs=HBM,
        out_shape=jax.ShapeDtypeStruct(shape, BF16),
        scratch_shapes=[
            pltpu.VMEM(shape, BF16),
            pltpu.SemaphoreType.DMA((4,)),
            pltpu.SemaphoreType.DMA((4,)),
        ],
        name="pack",
    )(step, forget, cot, fixed)


def join_kernel(in_ref, out_ref, sem):
    copies = [
        pltpu.make_async_copy(in_ref.at[j], out_ref.at[:, pl.ds(j * 128, 128)], sem) for j in range(GROUPS)
    ]
    for c in copies:
        c.start()
    for c in copies:
        c.wait()


def join(x):
    return pl.pallas_call(
        join_kernel,
        in_specs=[full(x.shape)],
        out_specs=HBM,
        out_shape=jax.ShapeDtypeStruct((Q, GROUPS * 128), BF16),
        scratch_shapes=[pltpu.SemaphoreType.DMA],
        name="join",
    )(x)


def dot(a, b):
    return lax.dot_general(a, b, (((1,), (0,)), ((), ())), preferred_element_type=F32)


def dot_t(a, b):
    return lax.dot_general(a, b, (((1,), (1,)), ((), ())), preferred_element_type=F32)


def fetch_maps(pos_ref, pieces, maps_ref, sem):
    my_y, my_z = pos_ref[0], pos_ref[1]
    copies = []
    for dy in range(NY):
        for dz in range(NZ):
            if dy == 0:
                source = pieces[0].at[dz]
            elif dy == 1:
                source = pieces[1].at[dz]
            elif dy == 3:
                source = pieces[2].at[dz]
            else:
                source = pieces[3].at[dz] if dz < 4 else pieces[4].at[dz - 4]
            place = ((my_y + dy) % NY) * NZ + (my_z + dz) % NZ
            copies.append(pltpu.make_async_copy(source, maps_ref.at[place], sem))
    for c in copies:
        c.start()
    for c in copies:
        c.wait()


def constants():
    rows = lax.broadcasted_iota(jnp.int32, (Q, Q), 0)
    cols = lax.broadcasted_iota(jnp.int32, (Q, Q), 1)
    lower = (rows >= cols).astype(F32).astype(BF16)
    same = (rows == cols).astype(F32).astype(BF16)
    return rows <= cols, lower, same


def prepare(c, in_ref, maps_ref, rate_ref, consts, mat_ref, turn_ref, e_ref, g_ref, s_ref, m_ref):
    upper, lower, same = consts
    both = maps_ref[c]
    b_rows, c_rows = both[:N], both[N:]
    prod = dot_t(jnp.concatenate([b_rows, same], axis=0), c_rows)
    mat_ref[c, :, :N] = jnp.where(upper, prod[:Q], 0.0).astype(BF16)
    mat_ref[c, :, N:] = b_rows
    turn_ref[c] = prod[Q:].astype(BF16)
    rows = in_ref[c, Q : Q + EXTRA, :].astype(F32)

    def wide(first, second):
        return jnp.concatenate(
            [jnp.broadcast_to(rows[first : first + 1], (HEAD, Q)), jnp.broadcast_to(rows[second : second + 1], (HEAD, Q))],
            axis=0,
        ).astype(BF16)

    steps = jnp.concatenate([wide(0, 1), wide(2, 3)], axis=1)
    forgets = jnp.concatenate([wide(4, 4), wide(5, 5)], axis=1)
    lower_twice = jnp.concatenate([lower, lower], axis=1)
    same_twice = jnp.concatenate([same, same], axis=1)
    sums = dot_t(
        jnp.concatenate([lower_twice, same_twice], axis=0), jnp.concatenate([steps, forgets], axis=0)
    )
    step_sum, step_col, forget_sum = sums[:Q, :128], sums[Q:, :128], sums[:Q, 128:]
    log_decay = -(rate_ref[0:1, :] * step_sum + forget_sum)
    middle = 0.5 * log_decay[Q - 1 : Q, :]
    gap = log_decay - middle
    e_ref[c] = jnp.exp(gap)
    g_ref[c] = step_col * jnp.exp(-gap)
    if s_ref is not None:
        s_ref[c] = step_sum
    m_ref[c] = jnp.broadcast_to(jnp.exp(middle), (8, 128))


def series_kernel(pos_ref, in_ref, p0, p1, p2, p3, p4, rate_ref, out_ref, maps_ref, mat_ref, turn_ref, e_ref, g_ref, m_ref, v_ref, sum_ref, back_ref, sem):
    fetch_maps(pos_ref, (p0, p1, p2, p3, p4), maps_ref, sem)
    consts = constants()

    def prep(i, _):
        for j in range(PREP):
            prepare(i * PREP + j, in_ref, maps_ref, rate_ref, consts, mat_ref, turn_ref, e_ref, g_ref, None, m_ref)
        return 0

    lax.fori_loop(0, GROUPS // PREP, prep, 0)
    skip = rate_ref[1:2, :]
    for k in range(3):
        back_ref[...] = jnp.zeros((N, 128), F32)

        def step(i, _):
            groups = [GROUPS - 1 - (i * UNROLL + j) for j in range(UNROLL)]
            values = [(in_ref[c, :Q, :] if k == 0 else v_ref[c]).astype(F32) for c in groups]
            turned = [(e_ref[c] * v).astype(BF16) for c, v in zip(groups, values)]
            local = [dot(turn_ref[c], x) for c, x in zip(groups, turned)]
            back = back_ref[...]
            states = []
            for j, c in enumerate(groups):
                states.append(back.astype(BF16))
                scale = m_ref[c, 0:1, :] * m_ref[jnp.maximum(c - 1, 0), 0:1, :]
                back = scale * (back + local[j])
            back_ref[...] = back
            mixed = [
                dot(mat_ref[c], jnp.concatenate([x, b], axis=0)) for c, x, b in zip(groups, turned, states)
            ]
            fresh = [
                (g_ref[c] * r + skip * v).astype(BF16) for c, r, v in zip(groups, mixed, values)
            ]
            totals = [
                (v if k == 0 else sum_ref[c]) + n.astype(F32) for c, v, n in zip(groups, values, fresh)
            ]
            for c, n, t in zip(groups, fresh, totals):
                if k < 2:
                    v_ref[c] = n
                    sum_ref[c] = t
                else:
                    out_ref[c] = t.astype(BF16)
            return 0

        lax.fori_loop(0, GROUPS // UNROLL, step, 0)


def rate_kernel(pos_ref, in_ref, sum_ref, p0, p1, p2, p3, p4, rate_ref, out_ref, maps_ref, mat_ref, turn_ref, e_ref, g_ref, s_ref, m_ref, back_ref, acc_ref, sem):
    fetch_maps(pos_ref, (p0, p1, p2, p3, p4), maps_ref, sem)
    consts = constants()

    def prep(i, _):
        for j in range(PREP):
            prepare(i * PREP + j, in_ref, maps_ref, rate_ref, consts, mat_ref, turn_ref, e_ref, g_ref, s_ref, m_ref)
        return 0

    lax.fori_loop(0, GROUPS // PREP, prep, 0)
    back_ref[...] = jnp.zeros((N, 256), F32)
    acc_ref[...] = jnp.zeros((2, 8, 128), F32)

    def step(i, _):
        groups = [GROUPS - 1 - (i * PAIRED + j) for j in range(PAIRED)]
        values = [sum_ref[c].astype(F32) for c in groups]
        turned = []
        for c, v in zip(groups, values):
            ev = e_ref[c] * v
            turned.append(jnp.concatenate([ev.astype(BF16), (ev * s_ref[c]).astype(BF16)], axis=1))
        local = [dot(turn_ref[c], x) for c, x in zip(groups, turned)]
        back, tangent = back_ref[:, :128], back_ref[:, 128:]
        states = []
        for j, c in enumerate(groups):
            tangent = tangent + s_ref[c, Q - 1 : Q, :] * back
            states.append(jnp.concatenate([back.astype(BF16), tangent.astype(BF16)], axis=1))
            scale = m_ref[c, 0:1, :] * m_ref[jnp.maximum(c - 1, 0), 0:1, :]
            back = scale * (back + local[j][:, :128])
            tangent = scale * (tangent + local[j][:, 128:])
        back_ref[:, :128] = back
        back_ref[:, 128:] = tangent
        mixed = [dot(mat_ref[c], jnp.concatenate([x, b], axis=0)) for c, x, b in zip(groups, turned, states)]
        rate_sum, skip_sum = acc_ref[0], acc_ref[1]
        for c, v, r in zip(groups, values, mixed):
            z = in_ref[c, Q + EXTRA :, :].astype(F32)
            change = g_ref[c] * (r[:, 128:] - s_ref[c] * r[:, :128])
            rate_sum = rate_sum + jnp.sum((z * change).reshape(16, 8, 128), axis=0)
            skip_sum = skip_sum + jnp.sum((z * v).reshape(16, 8, 128), axis=0)
        acc_ref[0] = rate_sum
        acc_ref[1] = skip_sum
        return 0

    lax.fori_loop(0, GROUPS // PAIRED, step, 0)
    lane = lax.broadcasted_iota(jnp.int32, (8, 128), 1)
    first = (pos_ref[0] * NZ + pos_ref[1]) * 2
    result = jnp.zeros((8, 128), F32)
    for kind in range(2):
        for head in range(2):
            picked = jnp.where((lane >= HEAD) if head else (lane < HEAD), acc_ref[kind], 0.0)
            value = jnp.sum(picked, keepdims=True)
            value = -value if kind == 0 else value
            result = jnp.where(lane == kind * H + first + head, value, result)
    out_ref[...] = result


def table_scratch(with_sums):
    square = pltpu.VMEM((GROUPS, Q, 128), F32)
    return [
        pltpu.VMEM((GROUPS, 2 * N, 128), BF16),
        pltpu.VMEM((GROUPS, Q, 256), BF16),
        pltpu.VMEM((GROUPS, N, Q), BF16),
        square,
        square,
        *([square] if with_sums else []),
        pltpu.VMEM((GROUPS, 8, 128), F32),
    ]


def series(pos, rows, pieces, rate):
    return pl.pallas_call(
        series_kernel,
        grid=(1,),
        in_specs=[SMEM, full((GROUPS, Q + EXTRA, 128)), HBM, HBM, HBM, HBM, HBM, full(rate.shape)],
        out_specs=full((GROUPS, Q, 128)),
        out_shape=jax.ShapeDtypeStruct((GROUPS, Q, 128), BF16),
        scratch_shapes=[
            *table_scratch(False),
            pltpu.VMEM((GROUPS, Q, 128), BF16),
            pltpu.VMEM((GROUPS, Q, 128), F32),
            pltpu.VMEM((N, 128), F32),
            pltpu.SemaphoreType.DMA,
        ],
        name="series",
        cost_estimate=pl.CostEstimate(flops=3_000_000_000, transcendentals=1_000_000, bytes_accessed=5_000_000),
    )(pos, rows, *pieces, rate)


def rates(pos, rows, summed, pieces, rate):
    return pl.pallas_call(
        rate_kernel,
        in_specs=[SMEM, full(rows.shape), full(summed.shape), HBM, HBM, HBM, HBM, HBM, full(rate.shape)],
        out_specs=full((8, 128)),
        out_shape=jax.ShapeDtypeStruct((8, 128), F32),
        scratch_shapes=[
            *table_scratch(True),
            pltpu.VMEM((N, 256), F32),
            pltpu.VMEM((2, 8, 128), F32),
            pltpu.SemaphoreType.DMA,
        ],
        name="rates",
        cost_estimate=pl.CostEstimate(flops=2_000_000_000, transcendentals=1_000_000, bytes_accessed=5_000_000),
    )(pos, rows, summed, *pieces, rate)


def assemble_kernel(own_ref, after_ref, far_after_ref, far_last_ref, last_ref, out_ref):
    out_ref[0] = own_ref[...]
    out_ref[1] = after_ref[...]
    out_ref[2] = far_after_ref[0 : 2 * N]
    out_ref[3] = far_after_ref[2 * N : 4 * N]
    out_ref[4, :N] = far_last_ref[0:N]
    out_ref[4, N:] = far_after_ref[4 * N : 5 * N]
    out_ref[5] = far_last_ref[N : 3 * N]
    out_ref[6] = far_last_ref[3 * N : 5 * N]
    out_ref[7] = last_ref[...]


def assemble(*parts):
    return pl.pallas_call(
        assemble_kernel,
        in_specs=[full(p.shape) for p in parts],
        out_specs=full((NZ, 2 * N, 128)),
        out_shape=jax.ShapeDtypeStruct((NZ, 2 * N, 128), BF16),
        name="assemble",
    )(*parts)


def gather_line(input_map, output_map):
    own = jnp.concatenate([input_map, output_map], axis=0)
    last, after = shifted(own, "seq_1", 1), shifted(own, "seq_1", -1)
    far_last = shifted(jnp.concatenate([last[:N], own, after]), "seq_1", 3)
    far_after = shifted(jnp.concatenate([last, own, after[N:]]), "seq_1", -3)
    return assemble(own, after, far_after, far_last, last)


def gather_plane(line):
    from_next = shifted(line, "seq_0", -1)
    from_last = shifted(line, "seq_0", 1)
    low = shifted(from_last[:4], "seq_0", 1)
    high = shifted(from_next[4:], "seq_0", -1)
    return line, from_next, from_last, low, high


def inner(cotangent, fixed_point, input_map, output_map, step_size, forget, decay_rate, skip_gain):
    my_y, my_z = lax.axis_index("seq_0"), lax.axis_index("seq_1")
    pos = jnp.stack([my_y, my_z]).astype(jnp.int32)
    first = (my_y * NZ + my_z) * 2
    own = jnp.stack([lax.dynamic_slice_in_dim(a, first, 2) for a in (decay_rate, skip_gain)])
    rate = jnp.repeat(own, HEAD, axis=1)

    line = gather_line(input_map[0], output_map[0])
    packed = pack(cotangent[0], fixed_point[0], step_size[0], forget)
    pieces = gather_plane(line)
    rows = lax.all_to_all(packed, SEQ, split_axis=0, concat_axis=0, tiled=True)
    summed = series(pos, rows, pieces, rate)
    result = lax.all_to_all(summed, SEQ, split_axis=0, concat_axis=0, tiled=True)
    totals = rates(pos, rows, summed, pieces, rate)
    for axis in BATCH:
        bit = 1
        while bit < lax.axis_size(axis):
            totals = totals + swapped(totals, axis, bit)
            bit *= 2
    copies = jnp.broadcast_to(totals[:1], (GROUPS, 1, 128))
    totals = lax.all_to_all(copies, SEQ, split_axis=0, concat_axis=0, tiled=True)
    totals = jnp.sum(totals, axis=(0, 1)) * (1.0 / (lax.axis_size(BATCH) * Q * GROUPS))
    return join(result)[None], totals[:H], totals[H:]


def solution(mesh):
    torus = Mesh(mesh.devices.reshape(4, 2, 4, 8), ("batch_0", "batch_1", "seq_0", "seq_1"))
    return jax.shard_map(
        inner,
        mesh=torus,
        in_specs=(
            P(BATCH, SEQ, None),
            P(BATCH, SEQ, None),
            P(BATCH, SEQ, None),
            P(BATCH, SEQ, None),
            P(BATCH, None, SEQ),
            P(BATCH, SEQ),
            P(),
            P(),
        ),
        out_specs=(P(BATCH, SEQ, None), P(), P()),
        check_vma=False,
    )
```
